256 devices in a mesh: gz: 64 (over z_hi, x, y), gx: 4 (over z_lo, core).
Axes of the slice: x: 4, y: 4, z: 8 (z_hi: 4, z_lo: 2; z = z_hi * 2 + z_lo), core: 2. Of those that a mesh axis runs over, the one named last changes fastest.
Arguments:
- density: float32 [512, 128, 128], P('gz', 'gx'), may hold values from -6 to 6
- velocity: float32 [3, 512, 128, 128], P(None, 'gz', 'gx'), may hold values from -6 to 6
- labels: int32 [512, 128, 128], P('gz', 'gx'), may hold values from 0 to 7
- sound_table: float32 [8], replicated, may hold values from 0.8 to 1.6
- mass_table: float32 [8], replicated, may hold values from 0.8 to 2
- source_index: int32 [4096], replicated, may hold values from 0 to 8388607
- source_values: float32 [1, 4096], replicated, may hold values from -6 to 6
Outputs:
- new_density: float32 [512, 128, 128], P('gz', 'gx')
- new_velocity: float32 [3, 512, 128, 128], P(None, 'gz', 'gx')
The draws below stay inside these ranges and needn't reach their ends.
Inputs may be any that keep to these rules, and one draw needn't show every extreme that they name: `source_index`: flat cell index z * 128 * 128 + x * 128 + y; an index may repeat.
All inputs are finite; a program needn't handle non-finite values.
Results may differ from the reference program's by a relative error of at most 0.00011.
Values sent between devices are 32-bit elements; how exact they have to be, the bound alone decides.
A program may use at most 64 MiB of HBM per device.

```python
import math
import jax
import jax.numpy as jnp

NZ = 512
NX = 128
NY = 128
LABELS = 8
PML_W = 20
STEPS = 1
SRC = 4096


def with_ends(drawn, key, smallest, top_value):
    longest = drawn.shape.index(max(drawn.shape))
    spots = []
    for shift in (0, 1):
        where = [jax.random.randint(jax.random.fold_in(key, axis), (), 0, length) for axis, length in enumerate(drawn.shape)]
        where[longest] = (where[longest] + shift) % drawn.shape[longest]
        spots.append(tuple(where))
    return drawn.at[spots[0]].set(smallest).at[spots[1]].set(top_value)


def level_of(stream_key, extent, shards, low, top_value):
    def one(position, shards_of):
        heights = jax.random.uniform(jax.random.fold_in(jax.random.fold_in(stream_key, 6), position), (shards_of,), jnp.float32, low / len(shards), top_value / len(shards))
        return jnp.repeat(jnp.exp(heights), extent[position] // shards_of).reshape((-1,) + (1,) * (len(extent) - position - 1))

    factor_of = one(*shards[0])
    for cut in shards[1:]:
        factor_of = factor_of * one(*cut)
    return factor_of


def gaussian(stream_key, dims, width, reach, shards=(), kind=jnp.bfloat16):
    drawn = jax.random.normal(stream_key, dims, jnp.float32) * width
    if len(shards) > 0:
        drawn = level_of(stream_key, dims, shards, -0.22, 0.18) * drawn
    return jnp.clip(drawn, min=-reach, max=reach).astype(kind)


def setup_inputs(seed: int = 0) -> dict:
    seeds = jax.random.split(jax.random.key(seed), 8)
    density = gaussian(seeds[0], (NZ, NX, NY), 1.0, 6.0, ((0, 64), (1, 4)), jnp.float32)
    velocity = gaussian(seeds[1], (3, NZ, NX, NY), 1.0, 6.0, ((1, 64), (2, 4)), jnp.float32)
    labels = with_ends(jax.random.randint(seeds[2], (NZ, NX, NY), 0, LABELS), jax.random.fold_in(seeds[2], 1), 0, LABELS - 1).astype(jnp.int32)
    sound_table = jnp.clip(jax.random.uniform(seeds[3], (LABELS,), jnp.float32, 0.8, 1.6), 0.8, 1.6)
    mass_table = jnp.clip(jax.random.uniform(seeds[4], (LABELS,), jnp.float32, 0.8, 2.0), 0.8, 2.0)
    source_index = with_ends(jax.random.randint(seeds[5], (SRC,), 0, NX * NY * NZ), jax.random.fold_in(seeds[5], 1), 0, (NX * NY * NZ) - 1).astype(jnp.int32)
    source_values = gaussian(seeds[6], (STEPS, SRC), 1.0, 6.0, (), jnp.float32)
    return {"density": density, "velocity": velocity, "labels": labels, "sound_table": sound_table, "mass_table": mass_table, "source_index": source_index, "source_values": source_values}


time_step = 0.3
absorb = 2.0

def wavenumber(length):
    positions = jnp.arange(length, dtype=jnp.int32)
    signed = jnp.where(positions < length // 2, positions, positions - length)
    return 2.0 * math.pi / length * signed.astype(jnp.float32)

def damping(length, speed_ref):
    coordinate = jnp.arange(length, dtype=jnp.int32).astype(jnp.float32)
    layer_depth = jnp.maximum(jnp.maximum(PML_W - coordinate, coordinate - (length - 1 - PML_W)), 0.0) / PML_W
    return jnp.exp(-absorb * speed_ref * layer_depth ** 4 * time_step * 0.5)

def reference(density, velocity, labels, sound_table, mass_table, source_index, source_values):
    speed_sq = sound_table[labels] ** 2
    rho_zero = mass_table[labels]
    speed_ref = jnp.max(sound_table)
    wave_list = (wavenumber(NZ)[:, None, None], wavenumber(NX)[None, :, None], wavenumber(NY)[None, None, :])
    magnitude = jnp.sqrt(wave_list[0] ** 2 + wave_list[1] ** 2 + wave_list[2] ** 2)
    correction = jnp.sinc(speed_ref * magnitude * time_step / (2.0 * math.pi))
    damp_list = (damping(NZ, speed_ref)[:, None, None], damping(NX, speed_ref)[None, :, None], damping(NY, speed_ref)[None, None, :])
    damp_all = damp_list[0] * damp_list[1] * damp_list[2]
    for moment in range(STEPS):
        pressure = speed_sq * density
        spectrum = jnp.fft.fftn(pressure) * correction
        updated = []
        for direction in range(3):
            factor = 1j * wave_list[direction] * jnp.exp(0.5j * wave_list[direction])
            gradient_part = jnp.real(jnp.fft.ifftn(spectrum * factor))
            updated.append(damp_list[direction] * (damp_list[direction] * velocity[direction] - time_step / rho_zero * gradient_part))
        velocity = jnp.stack(updated)
        summed = None
        for direction in range(3):
            factor = 1j * wave_list[direction] * jnp.exp(-0.5j * wave_list[direction])
            contribution = jnp.fft.fftn(velocity[direction]) * factor
            summed = contribution if summed is None else summed + contribution
        spread = jnp.real(jnp.fft.ifftn(summed * correction))
        density = damp_all * (damp_all * density - time_step * rho_zero * spread)
        density = density.reshape(-1).at[source_index].add(source_values[moment]).reshape(density.shape)
    return (density, velocity)
```

```python
import math

import jax
import jax.numpy as jnp
import numpy as np
from jax import lax
from jax.experimental import pallas as pl
from jax.experimental.pallas import tpu as pltpu
from jax.sharding import PartitionSpec as P

NZ = 512
NX = 128
NY = 128
LABELS = 8
PML_W = 20
SRC = 4096
DT = 0.3
ABSORB = 2.0
G = 16
Z_LOC = 8
X_LOC = 32
ROWS = Z_LOC * X_LOC
MESH = pl.DeviceIdType.MESH
F32 = jnp.float32
BF16 = jnp.bfloat16

P_A, P_B, W0_B, WZ_B, U0_A, UX_A, UZ_A, VY_A, VX_A, VZ_A, QXY_B, QZ_B, S_B, S_A = range(14)


def basis(n):
    j = np.arange(n)
    f = np.concatenate([np.arange(n // 2 + 1), np.arange(1, n // 2)])
    is_sin = (np.arange(n) > n // 2)[:, None]
    scale = np.where((f == 0) | (f == n // 2), math.sqrt(1.0 / n), math.sqrt(2.0 / n))[:, None]
    k = (2.0 * math.pi / n * f)[:, None]
    phase = 2.0 * math.pi / n * ((f[:, None] * j[None, :]) % n)
    half = 2.0 * math.pi / (2 * n) * ((f[:, None] * (2 * j[None, :] + 1)) % (2 * n))
    forward = np.where(is_sin, np.sin(phase), np.cos(phase)) * scale
    slope = np.where(is_sin, k * np.cos(half), -k * np.sin(half)) * scale
    return forward, slope


def parts(table):
    table = table.astype(np.float32)
    high = table.astype(jnp.bfloat16)
    low = (table - high.astype(np.float32)).astype(jnp.bfloat16)
    return [high, low]


def tables():
    r, d = basis(NX)
    small = np.stack(parts(r) + parts(d))
    r, d = basis(NZ)
    lane = np.arange(NZ)
    z = (lane % 4) * 128 + (lane // 32) * Z_LOC + (lane % 32) // 4
    large = np.stack(parts(r[:, z]) + parts(d[:, z]))
    return small, large


def split(x):
    high = x.astype(BF16)
    return high, (x - high.astype(F32)).astype(BF16)


def product(a, b, dims):
    contract = (((1,), (0 if dims == "nn" else 1,)), ((), ()))

    def dot(u, v):
        return lax.dot_general(u, v, contract, preferred_element_type=F32)

    return dot(a[0], b[0]) + dot(a[1], b[0]) + dot(a[0], b[1])


def swap_blocks(a):
    lane = lax.broadcasted_iota(jnp.int32, a[0].shape, 1)
    low_half = lane < 64
    even = (lane % 64) < 32

    def far(u, v):
        return (
            jnp.where(low_half, u, pltpu.roll(v, 64, 1)),
            jnp.where(low_half, pltpu.roll(u, 64, 1), v),
        )

    def near(u, v):
        return (
            jnp.where(even, u, pltpu.roll(v, 32, 1)),
            jnp.where(even, pltpu.roll(u, 96, 1), v),
        )

    c0, c2 = far(a[0], a[2])
    c1, c3 = far(a[1], a[3])
    b0, b1 = near(c0, c1)
    b2, b3 = near(c2, c3)
    return b0, b1, b2, b3


def kernel(
    sound, mass, dens_hbm, vel_hbm, lab_hbm, sidx, sval, small, large_hbm,
    out_d, out_v,
    send_buf, recv_buf, work, long_a, long_b, dens, vel, lab, large,
    base_v, coef_v, base_d, coef_d, corr, row_of, col_of,
    send_sem, recv_sem, load_sem, out_sem,
):
    gz = lax.axis_index("gz")
    gx = lax.axis_index("gx")
    z_hi = lax.div(gz, 16)
    me_b = lax.rem(gz, 16)
    me_a = z_hi * 4 + gx

    def device_of(group, peer):
        if group == "A":
            return (lax.div(peer, 4) * 16 + me_b, lax.rem(peer, 4))
        return (z_hi * 16 + peer, gx)

    loads = [
        pltpu.make_async_copy(lab_hbm, lab, load_sem.at[0]),
        pltpu.make_async_copy(dens_hbm, dens, load_sem.at[1]),
        pltpu.make_async_copy(vel_hbm, vel, load_sem.at[2]),
        pltpu.make_async_copy(large_hbm, large, load_sem.at[3]),
    ]
    for load in loads:
        load.start()

    barrier = pltpu.get_barrier_semaphore()

    def greet(step, carry):
        for group, me in (("A", me_a), ("B", me_b)):
            peer = lax.rem(me + step, G)
            pl.semaphore_signal(
                barrier, inc=1, device_id=device_of(group, peer), device_id_type=MESH
            )
        return carry

    lax.fori_loop(1, G, greet, 0)

    def send(which, group):
        me = me_a if group == "A" else me_b
        recv_buf[which, me] = send_buf[which, me]

        def one(step, carry):
            peer = lax.rem(me + step, G)
            pltpu.make_async_remote_copy(
                send_buf.at[which, peer],
                recv_buf.at[which, me],
                send_sem.at[which],
                recv_sem.at[which],
                device_id=device_of(group, peer),
                device_id_type=MESH,
            ).start()
            return carry

        lax.fori_loop(1, G, one, 0)

    def whole(which):
        return pltpu.make_async_copy(
            send_buf.at[which, pl.ds(0, G - 1)],
            recv_buf.at[which, pl.ds(0, G - 1)],
            recv_sem.at[which],
        )

    def arrived(which):
        whole(which).wait()

    def sent(which):
        pltpu.make_async_copy(
            send_buf.at[which, pl.ds(0, G - 1)],
            recv_buf.at[which, pl.ds(0, G - 1)],
            send_sem.at[which],
        ).wait()

    r_small = (small[0], small[1])
    d_small = (small[2], small[3])

    def put(which, value):
        send_buf[which] = value.reshape(G, 8, ROWS)

    def to_x_lines(which):
        got = recv_buf[which].reshape(4, 4, 8, ROWS)
        for tile in range(2):
            a = [got[:, g, :, tile * 128 : tile * 128 + 128].reshape(32, 128) for g in range(4)]
            for q, b in enumerate(swap_blocks(a)):
                work[pl.ds((tile * 4 + q) * 32, 32), :] = b
        return jnp.concatenate([work[pl.ds(ky, 32, stride=8), :] for ky in range(8)], axis=0)

    def from_x_lines(which, value):
        for ky in range(8):
            work[pl.ds(ky, 32, stride=8), :] = value[ky * 32 : ky * 32 + 32]
        for tile in range(2):
            b = [work[pl.ds((tile * 4 + q) * 32, 32), :] for q in range(4)]
            for g, a in enumerate(swap_blocks(b)):
                a = a.reshape(4, 8, 128)
                for high in range(4):
                    send_buf[which, high * 4 + g, :, tile * 128 : tile * 128 + 128] = a[high]

    def to_z_lines(which, place):
        got = recv_buf[which].reshape(4, 4, 8, ROWS)
        for tile in range(2):
            a = [got[:, g, :, tile * 128 : tile * 128 + 128].reshape(32, 128) for g in range(4)]
            for q, b in enumerate(swap_blocks(a)):
                b = b.reshape(4, 8, 128)
                for high in range(4):
                    place[(tile * 4 + q) * 8 : (tile * 4 + q) * 8 + 8, high * 128 : high * 128 + 128] = b[high]
        return place[...]

    def from_z_lines(which, value):
        for tile in range(2):
            b = []
            for q in range(4):
                rows = value[(tile * 4 + q) * 8 : (tile * 4 + q) * 8 + 8]
                b.append(jnp.concatenate([rows[:, h * 128 : h * 128 + 128] for h in range(4)], axis=0))
            for g, a in enumerate(swap_blocks(b)):
                a = a.reshape(4, 8, 128)
                for high in range(4):
                    send_buf[which, high * 4 + g, :, tile * 128 : tile * 128 + 128] = a[high]

    def turned(which):
        return split(recv_buf[which].reshape(G * 8, ROWS).T)

    speed_ref = sound[0]
    for tissue in range(1, LABELS):
        speed_ref = jnp.maximum(speed_ref, sound[tissue])

    loads[0].wait()
    loads[1].wait()
    classes = lab[...].reshape(ROWS, NY)
    speed = jnp.full((ROWS, NY), sound[0])
    for tissue in range(1, LABELS):
        speed = jnp.where(classes == tissue, sound[tissue], speed)
    pressure = speed * speed * dens[...].reshape(ROWS, NY)
    put(P_A, product(r_small, split(pressure), "nt"))
    pl.semaphore_wait(barrier, 2 * (G - 1))
    send(P_A, "A")

    loads[2].wait()
    density_mass = jnp.full((ROWS, NY), mass[0])
    for tissue in range(1, LABELS):
        density_mass = jnp.where(classes == tissue, mass[tissue], density_mass)
    row = lax.broadcasted_iota(jnp.int32, (ROWS, NY), 0)
    col = lax.broadcasted_iota(jnp.int32, (ROWS, NY), 1)

    def damping(position, length):
        coordinate = position.astype(F32)
        depth = jnp.maximum(
            jnp.maximum(PML_W - coordinate, coordinate - (length - 1 - PML_W)), 0.0
        ) / PML_W
        square = depth * depth
        return jnp.exp(-ABSORB * speed_ref * (square * square) * DT * 0.5)

    damp = (
        damping(gz * Z_LOC + row // X_LOC, NZ),
        damping(gx * X_LOC + row % X_LOC, NX),
        damping(col, NY),
    )
    over_mass = DT / density_mass
    for a in range(3):
        base_v[a] = damp[a] * (damp[a] * vel[a].reshape(ROWS, NY))
        coef_v[a] = damp[a] * over_mass
    damp_all = damp[0] * damp[1] * damp[2]
    base_d[...] = damp_all * (damp_all * dens[...].reshape(ROWS, NY))
    coef_d[...] = damp_all * (DT * density_mass)

    line = lax.broadcasted_iota(jnp.int32, (64, NZ), 0)
    index_z = lax.broadcasted_iota(jnp.int32, (64, NZ), 1)

    def wave(index, length):
        folded = jnp.where(index <= length // 2, index, index - length // 2)
        return folded.astype(F32) * (2.0 * math.pi / length)

    wz = wave(index_z, NZ)
    wx = wave(me_b * 8 + line % 8, NX)
    wy = wave(me_a * 8 + line // 8, NY)
    angle = speed_ref * jnp.sqrt(wz * wz + wx * wx + wy * wy) * (DT / 2.0)
    at_zero = angle == 0.0
    safe = jnp.where(at_zero, 1.0, angle)
    corr[...] = jnp.where(at_zero, 1.0, jnp.sin(safe) / safe)

    arrived(P_A)
    put(P_B, product(r_small, split(to_x_lines(P_A)), "nt"))
    send(P_B, "B")

    where = sidx[...]
    plane = NX * NY
    z_off = where // plane - gz * Z_LOC
    remain = where % plane
    x_off = remain // NY - gx * X_LOC
    inside = (z_off >= 0) & (z_off < Z_LOC) & (x_off >= 0) & (x_off < X_LOC)
    row_of[...] = jnp.where(inside, z_off * X_LOC + x_off, -1)
    col_of[...] = remain % NY

    def add_some(step, carry):
        picks = []
        highs = []
        lows = []
        for part in range(2):
            at = pl.ds(step * 2 + part, 1)
            picks.append(jnp.where(row == row_of[at, :], 1.0, 0.0).astype(BF16))
            amount = jnp.where(row[:NY] == col_of[at, :], sval[at, :], 0.0)
            high, low = split(amount)
            highs.append(high)
            lows.append(low)
        pick = jnp.concatenate(picks, axis=1)
        contract = (((1,), (1,)), ((), ()))
        high = lax.dot_general(pick, jnp.concatenate(highs, axis=1), contract, preferred_element_type=F32)
        low = lax.dot_general(pick, jnp.concatenate(lows, axis=1), contract, preferred_element_type=F32)
        base_d[...] += high + low
        return carry

    lax.fori_loop(0, SRC // NY // 2, add_some, 0)

    loads[3].wait()
    r_large = (large[0], large[1])
    d_large = (large[2], large[3])

    arrived(P_B)
    spectrum = product(split(to_z_lines(P_B, long_a)), r_large, "nt")
    spectrum = split(spectrum * corr[...])
    from_z_lines(W0_B, product(spectrum, r_large, "nn"))
    send(W0_B, "B")
    from_z_lines(WZ_B, product(spectrum, d_large, "nn"))
    send(WZ_B, "B")

    arrived(W0_B)
    field = turned(W0_B)
    from_x_lines(U0_A, product(field, r_small, "nn"))
    send(U0_A, "A")
    from_x_lines(UX_A, product(field, d_small, "nn"))
    send(UX_A, "A")
    arrived(WZ_B)
    from_x_lines(UZ_A, product(turned(WZ_B), r_small, "nn"))
    send(UZ_A, "A")

    stores = []
    for came, goes, a, back, sign in (
        (U0_A, VY_A, 2, d_small, -1),
        (UX_A, VX_A, 1, r_small, 1),
        (UZ_A, VZ_A, 0, r_small, 1),
    ):
        arrived(came)
        slope = product(turned(came), back, "nn")
        fresh = base_v[a] - coef_v[a] * slope
        halves = split(fresh)
        if sign > 0:
            put(goes, product(r_small, halves, "nt"))
        else:
            put(goes, -product(d_small, halves, "nt"))
        send(goes, "A")
        vel[a] = fresh.reshape(Z_LOC, X_LOC, NY)
        store = pltpu.make_async_copy(vel.at[a], out_v.at[a], out_sem.at[a])
        store.start()
        stores.append(store)

    arrived(VY_A)
    part_y = product(r_small, split(to_x_lines(VY_A)), "nt")
    arrived(VX_A)
    put(QXY_B, part_y - product(d_small, split(to_x_lines(VX_A)), "nt"))
    send(QXY_B, "B")
    arrived(VZ_A)
    put(QZ_B, product(r_small, split(to_x_lines(VZ_A)), "nt"))
    send(QZ_B, "B")

    arrived(QXY_B)
    spectrum = product(split(to_z_lines(QXY_B, long_a)), r_large, "nt")
    arrived(QZ_B)
    spectrum = spectrum - product(split(to_z_lines(QZ_B, long_b)), d_large, "nt")
    from_z_lines(S_B, product(split(spectrum * corr[...]), r_large, "nn"))
    send(S_B, "B")

    arrived(S_B)
    from_x_lines(S_A, product(turned(S_B), r_small, "nn"))
    send(S_A, "A")

    arrived(S_A)
    spread = product(turned(S_A), r_small, "nn")
    dens[...] = (base_d[...] - coef_d[...] * spread).reshape(Z_LOC, X_LOC, NY)
    store = pltpu.make_async_copy(dens, out_d, out_sem.at[3])
    store.start()
    stores.append(store)
    for which in range(14):
        sent(which)
    for store in stores:
        store.wait()


def shards(density, velocity, labels, sound_table, mass_table, source_index, source_values):
    small, large = tables()
    block = (G, 8, ROWS)
    vmem = pl.BlockSpec(memory_space=pltpu.VMEM)
    smem = pl.BlockSpec(memory_space=pltpu.SMEM)
    anyspace = pl.BlockSpec(memory_space=pl.ANY)
    field = (Z_LOC, X_LOC, NY)
    return pl.pallas_call(
        kernel,
        out_shape=(
            jax.ShapeDtypeStruct(field, F32),
            jax.ShapeDtypeStruct((3,) + field, F32),
        ),
        in_specs=[smem, smem, anyspace, anyspace, anyspace, vmem, vmem, vmem, anyspace],
        out_specs=(anyspace, anyspace),
        scratch_shapes=[
            pltpu.VMEM((14,) + block, F32),
            pltpu.VMEM((14,) + block, F32),
            pltpu.VMEM((ROWS, NY), F32),
            pltpu.VMEM((64, NZ), F32),
            pltpu.VMEM((64, NZ), F32),
            pltpu.VMEM(field, F32),
            pltpu.VMEM((3,) + field, F32),
            pltpu.VMEM(field, jnp.int32),
            pltpu.VMEM((4, NZ, NZ), BF16),
            pltpu.VMEM((3, ROWS, NY), F32),
            pltpu.VMEM((3, ROWS, NY), F32),
            pltpu.VMEM((ROWS, NY), F32),
            pltpu.VMEM((ROWS, NY), F32),
            pltpu.VMEM((64, NZ), F32),
            pltpu.VMEM((SRC // NY, NY), jnp.int32),
            pltpu.VMEM((SRC // NY, NY), jnp.int32),
            pltpu.SemaphoreType.DMA((14,)),
            pltpu.SemaphoreType.DMA((14,)),
            pltpu.SemaphoreType.DMA((4,)),
            pltpu.SemaphoreType.DMA((4,)),
        ],
        compiler_params=pltpu.CompilerParams(collective_id=0, has_side_effects=True),
    )(
        sound_table,
        mass_table,
        density,
        velocity,
        labels,
        source_index.reshape(SRC // NY, NY),
        source_values[0].reshape(SRC // NY, NY),
        jnp.asarray(small),
        jnp.asarray(large),
    )


def solution(mesh):
    in_specs = (
        P("gz", "gx", None),
        P(None, "gz", "gx", None),
        P("gz", "gx", None),
        P(),
        P(),
        P(),
        P(),
    )
    out_specs = (P("gz", "gx", None), P(None, "gz", "gx", None))
    return jax.shard_map(shards, mesh=mesh, in_specs=in_specs, out_specs=out_specs, check_vma=False)
```

```python
import math

import jax
import jax.numpy as jnp
import numpy as np
from jax import lax
from jax.experimental import pallas as pl
from jax.experimental.pallas import tpu as pltpu
from jax.sharding import PartitionSpec as P

NZ = 512
NX = 128
NY = 128
LABELS = 8
PML_W = 20
SRC = 4096
DT = 0.3
ABSORB = 2.0
G = 16
Z_LOC = 8
X_LOC = 32
ROWS = Z_LOC * X_LOC
MESH = pl.DeviceIdType.MESH
F32 = jnp.float32
BF16 = jnp.bfloat16

P_A, P_B, W0_B, WZ_B, U0_A, UX_A, UZ_A, VY_A, VX_A, VZ_A, QXY_B, QZ_B, S_B, S_A = range(14)


def basis(n):
    j = np.arange(n)
    f = np.concatenate([np.arange(n // 2 + 1), np.arange(1, n // 2)])
    is_sin = (np.arange(n) > n // 2)[:, None]
    scale = np.where((f == 0) | (f == n // 2), math.sqrt(1.0 / n), math.sqrt(2.0 / n))[:, None]
    k = (2.0 * math.pi / n * f)[:, None]
    phase = 2.0 * math.pi / n * ((f[:, None] * j[None, :]) % n)
    half = 2.0 * math.pi / (2 * n) * ((f[:, None] * (2 * j[None, :] + 1)) % (2 * n))
    forward = np.where(is_sin, np.sin(phase), np.cos(phase)) * scale
    slope = np.where(is_sin, k * np.cos(half), -k * np.sin(half)) * scale
    return forward, slope


def parts(table):
    table = table.astype(np.float32)
    high = table.astype(jnp.bfloat16)
    low = (table - high.astype(np.float32)).astype(jnp.bfloat16)
    return [high, low]


def tables():
    r, d = basis(NX)
    small = np.stack(parts(r) + parts(d))
    r, d = basis(NZ)
    lane = np.arange(NZ)
    z = (lane % 4) * 128 + (lane // 32) * Z_LOC + (lane % 32) // 4
    large = np.stack(parts(r[:, z]) + parts(d[:, z]))
    return small, large


def split(x):
    high = x.astype(BF16)
    return high, (x - high.astype(F32)).astype(BF16)


def product(a, b, dims):
    contract = (((1,), (0 if dims == "nn" else 1,)), ((), ()))

    def dot(u, v):
        return lax.dot_general(u, v, contract, preferred_element_type=F32)

    return dot(a[0], b[0]) + dot(a[1], b[0]) + dot(a[0], b[1])


def swap_blocks(a):
    lane = lax.broadcasted_iota(jnp.int32, a[0].shape, 1)
    low_half = lane < 64
    even = (lane % 64) < 32

    def far(u, v):
        return (
            jnp.where(low_half, u, pltpu.roll(v, 64, 1)),
            jnp.where(low_half, pltpu.roll(u, 64, 1), v),
        )

    def near(u, v):
        return (
            jnp.where(even, u, pltpu.roll(v, 32, 1)),
            jnp.where(even, pltpu.roll(u, 96, 1), v),
        )

    c0, c2 = far(a[0], a[2])
    c1, c3 = far(a[1], a[3])
    b0, b1 = near(c0, c1)
    b2, b3 = near(c2, c3)
    return b0, b1, b2, b3


def kernel(
    sound_hbm, mass_hbm, dens_hbm, vel_hbm, lab_hbm, sidx_hbm, sval_hbm, small_hbm, large_hbm,
    out_d, out_v,
    send_buf, recv_buf, work, long_a, long_b, sound, mass, dens, vel, lab, sidx, sval, small, large,
    base_v, coef_v, base_d, coef_d, corr, row_of, col_of,
    send_sem, recv_sem, load_sem,
):
    gz = lax.axis_index("gz")
    gx = lax.axis_index("gx")
    z_hi = lax.div(gz, 16)
    me_b = lax.rem(gz, 16)
    me_a = z_hi * 4 + gx

    b_x, b_y = lax.div(me_b, 4), lax.rem(me_b, 4)
    far_b = sorted(
        [(x, y) for x in range(4) for y in range(4) if x or y],
        key=lambda o: -(min(o[0], 4 - o[0]) + min(o[1], 4 - o[1])),
    )
    peers = {
        "A": [lax.rem(me_a + o, G) for o in sorted(range(1, G), key=lambda o: abs(o - 8))],
        "B": [lax.rem(b_x + x, 4) * 4 + lax.rem(b_y + y, 4) for x, y in far_b],
    }

    def device_of(group, peer):
        if group == "A":
            return (lax.div(peer, 4) * 16 + me_b, lax.rem(peer, 4))
        return (z_hi * 16 + peer, gx)

    barrier = pltpu.get_barrier_semaphore()

    for pair in zip(peers["A"], peers["B"]):
        for group, peer in zip("AB", pair):
            pl.semaphore_signal(
                barrier, inc=1, device_id=device_of(group, peer), device_id_type=MESH
            )

    loads = [
        pltpu.make_async_copy(away, here, load_sem.at[i])
        for i, (away, here) in enumerate(
            (
                (sound_hbm, sound),
                (lab_hbm, lab),
                (dens_hbm, dens),
                (small_hbm, small),
                (mass_hbm, mass),
                (vel_hbm, vel),
                (sidx_hbm, sidx),
                (sval_hbm, sval),
                (large_hbm, large),
            )
        )
    ]
    for load in loads:
        load.start()

    def send(which, group):
        me = me_a if group == "A" else me_b
        recv_buf[which, me] = send_buf[which, me]

        for peer in peers[group]:
            pltpu.make_async_remote_copy(
                send_buf.at[which, peer],
                recv_buf.at[which, me],
                send_sem.at[which],
                recv_sem.at[which],
                device_id=device_of(group, peer),
                device_id_type=MESH,
            ).start()

    def whole(which):
        return pltpu.make_async_copy(
            send_buf.at[which, pl.ds(0, G - 1)],
            recv_buf.at[which, pl.ds(0, G - 1)],
            recv_sem.at[which],
        )

    def arrived(which):
        whole(which).wait()

    def sent(which):
        pltpu.make_async_copy(
            send_buf.at[which, pl.ds(0, G - 1)],
            recv_buf.at[which, pl.ds(0, G - 1)],
            send_sem.at[which],
        ).wait()

    def put(which, value):
        send_buf[which] = value.reshape(G, 8, ROWS)

    def to_x_lines(which):
        got = recv_buf[which].reshape(4, 4, 8, ROWS)
        for tile in range(2):
            a = [got[:, g, :, tile * 128 : tile * 128 + 128].reshape(32, 128) for g in range(4)]
            for q, b in enumerate(swap_blocks(a)):
                work[pl.ds((tile * 4 + q) * 32, 32), :] = b
        return jnp.concatenate([work[pl.ds(ky, 32, stride=8), :] for ky in range(8)], axis=0)

    def from_x_lines(which, value):
        for ky in range(8):
            work[pl.ds(ky, 32, stride=8), :] = value[ky * 32 : ky * 32 + 32]
        for tile in range(2):
            b = [work[pl.ds((tile * 4 + q) * 32, 32), :] for q in range(4)]
            for g, a in enumerate(swap_blocks(b)):
                a = a.reshape(4, 8, 128)
                for high in range(4):
                    send_buf[which, high * 4 + g, :, tile * 128 : tile * 128 + 128] = a[high]

    def to_z_lines(which, place):
        got = recv_buf[which].reshape(4, 4, 8, ROWS)
        for tile in range(2):
            a = [got[:, g, :, tile * 128 : tile * 128 + 128].reshape(32, 128) for g in range(4)]
            for q, b in enumerate(swap_blocks(a)):
                b = b.reshape(4, 8, 128)
                for high in range(4):
                    place[(tile * 4 + q) * 8 : (tile * 4 + q) * 8 + 8, high * 128 : high * 128 + 128] = b[high]
        return place[...]

    def from_z_lines(which, value):
        for tile in range(2):
            b = []
            for q in range(4):
                rows = value[(tile * 4 + q) * 8 : (tile * 4 + q) * 8 + 8]
                b.append(jnp.concatenate([rows[:, h * 128 : h * 128 + 128] for h in range(4)], axis=0))
            for g, a in enumerate(swap_blocks(b)):
                a = a.reshape(4, 8, 128)
                for high in range(4):
                    send_buf[which, high * 4 + g, :, tile * 128 : tile * 128 + 128] = a[high]

    def turned(which):
        return split(recv_buf[which].reshape(G * 8, ROWS).T)

    for load in loads[:4]:
        load.wait()
    r_small = (small[0], small[1])
    d_small = (small[2], small[3])
    speed_ref = sound[0]
    for tissue in range(1, LABELS):
        speed_ref = jnp.maximum(speed_ref, sound[tissue])

    classes = lab[...].reshape(ROWS, NY)
    speed = jnp.full((ROWS, NY), sound[0])
    for tissue in range(1, LABELS):
        speed = jnp.where(classes == tissue, sound[tissue], speed)
    pressure = speed * speed * dens[...].reshape(ROWS, NY)
    put(P_A, product(r_small, split(pressure), "nt"))
    pl.semaphore_wait(barrier, 2 * (G - 1))
    send(P_A, "A")

    for load in loads[4:8]:
        load.wait()
    density_mass = jnp.full((ROWS, NY), mass[0])
    for tissue in range(1, LABELS):
        density_mass = jnp.where(classes == tissue, mass[tissue], density_mass)
    row = lax.broadcasted_iota(jnp.int32, (ROWS, NY), 0)
    col = lax.broadcasted_iota(jnp.int32, (ROWS, NY), 1)

    def damping(position, length):
        coordinate = position.astype(F32)
        depth = jnp.maximum(
            jnp.maximum(PML_W - coordinate, coordinate - (length - 1 - PML_W)), 0.0
        ) / PML_W
        square = depth * depth
        return jnp.exp(-ABSORB * speed_ref * (square * square) * DT * 0.5)

    damp = (
        damping(gz * Z_LOC + row // X_LOC, NZ),
        damping(gx * X_LOC + row % X_LOC, NX),
        damping(col, NY),
    )
    over_mass = DT / density_mass
    for a in range(3):
        base_v[a] = damp[a] * (damp[a] * vel[a].reshape(ROWS, NY))
        coef_v[a] = damp[a] * over_mass
    damp_all = damp[0] * damp[1] * damp[2]
    base_d[...] = damp_all * (damp_all * dens[...].reshape(ROWS, NY))
    coef_d[...] = damp_all * (DT * density_mass)

    line = lax.broadcasted_iota(jnp.int32, (64, NZ), 0)
    index_z = lax.broadcasted_iota(jnp.int32, (64, NZ), 1)

    def wave(index, length):
        folded = jnp.where(index <= length // 2, index, index - length // 2)
        return folded.astype(F32) * (2.0 * math.pi / length)

    wz = wave(index_z, NZ)
    wx = wave(me_b * 8 + line % 8, NX)
    wy = wave(me_a * 8 + line // 8, NY)
    angle = speed_ref * jnp.sqrt(wz * wz + wx * wx + wy * wy) * (DT / 2.0)
    at_zero = angle == 0.0
    safe = jnp.where(at_zero, 1.0, angle)
    corr[...] = jnp.where(at_zero, 1.0, jnp.sin(safe) / safe)

    arrived(P_A)
    put(P_B, product(r_small, split(to_x_lines(P_A)), "nt"))
    send(P_B, "B")

    where = sidx[...]
    plane = NX * NY
    z_off = where // plane - gz * Z_LOC
    remain = where % plane
    x_off = remain // NY - gx * X_LOC
    inside = (z_off >= 0) & (z_off < Z_LOC) & (x_off >= 0) & (x_off < X_LOC)
    row_of[...] = jnp.where(inside, z_off * X_LOC + x_off, -1)
    col_of[...] = remain % NY

    def add_some(step, carry):
        picks = []
        highs = []
        lows = []
        for part in range(2):
            at = pl.ds(step * 2 + part, 1)
            picks.append(jnp.where(row == row_of[at, :], 1.0, 0.0).astype(BF16))
            amount = jnp.where(row[:NY] == col_of[at, :], sval[at, :], 0.0)
            high, low = split(amount)
            highs.append(high)
            lows.append(low)
        pick = jnp.concatenate(picks, axis=1)
        contract = (((1,), (1,)), ((), ()))
        high = lax.dot_general(pick, jnp.concatenate(highs, axis=1), contract, preferred_element_type=F32)
        low = lax.dot_general(pick, jnp.concatenate(lows, axis=1), contract, preferred_element_type=F32)
        base_d[...] += high + low
        return carry

    lax.fori_loop(0, SRC // NY // 2, add_some, 0)

    loads[8].wait()
    r_large = (large[0], large[1])
    d_large = (large[2], large[3])

    arrived(P_B)
    spectrum = product(split(to_z_lines(P_B, long_a)), r_large, "nt")
    spectrum = split(spectrum * corr[...])
    from_z_lines(W0_B, product(spectrum, r_large, "nn"))
    send(W0_B, "B")
    from_z_lines(WZ_B, product(spectrum, d_large, "nn"))
    send(WZ_B, "B")

    arrived(W0_B)
    field = turned(W0_B)
    from_x_lines(U0_A, product(field, r_small, "nn"))
    send(U0_A, "A")
    from_x_lines(UX_A, product(field, d_small, "nn"))
    send(UX_A, "A")
    arrived(WZ_B)
    from_x_lines(UZ_A, product(turned(WZ_B), r_small, "nn"))
    send(UZ_A, "A")

    for came, goes, a, back, sign in (
        (U0_A, VY_A, 2, d_small, -1),
        (UX_A, VX_A, 1, r_small, 1),
        (UZ_A, VZ_A, 0, r_small, 1),
    ):
        arrived(came)
        slope = product(turned(came), back, "nn")
        fresh = base_v[a] - coef_v[a] * slope
        halves = split(fresh)
        if sign > 0:
            put(goes, product(r_small, halves, "nt"))
        else:
            put(goes, -product(d_small, halves, "nt"))
        send(goes, "A")
        out_v[a] = fresh.reshape(Z_LOC, X_LOC, NY)

    arrived(VY_A)
    part_y = product(r_small, split(to_x_lines(VY_A)), "nt")
    arrived(VX_A)
    put(QXY_B, part_y - product(d_small, split(to_x_lines(VX_A)), "nt"))
    send(QXY_B, "B")
    arrived(VZ_A)
    put(QZ_B, product(r_small, split(to_x_lines(VZ_A)), "nt"))
    send(QZ_B, "B")

    arrived(QXY_B)
    spectrum = product(split(to_z_lines(QXY_B, long_a)), r_large, "nt")
    arrived(QZ_B)
    spectrum = spectrum - product(split(to_z_lines(QZ_B, long_b)), d_large, "nt")
    from_z_lines(S_B, product(split(spectrum * corr[...]), r_large, "nn"))
    send(S_B, "B")

    arrived(S_B)
    from_x_lines(S_A, product(turned(S_B), r_small, "nn"))
    send(S_A, "A")

    arrived(S_A)
    spread = product(turned(S_A), r_small, "nn")
    out_d[...] = (base_d[...] - coef_d[...] * spread).reshape(Z_LOC, X_LOC, NY)
    for which in range(14):
        sent(which)


def shards(density, velocity, labels, sound_table, mass_table, source_index, source_values):
    small, large = tables()
    block = (G, 8, ROWS)
    vmem = pl.BlockSpec(memory_space=pltpu.VMEM)
    hbm = pl.BlockSpec(memory_space=pl.ANY)
    field = (Z_LOC, X_LOC, NY)
    return pl.pallas_call(
        kernel,
        out_shape=(
            pltpu.VMEM(field, F32),
            pltpu.VMEM((3,) + field, F32),
        ),
        in_specs=[hbm] * 9,
        out_specs=(vmem, vmem),
        scratch_shapes=[
            pltpu.VMEM((14,) + block, F32),
            pltpu.VMEM((14,) + block, F32),
            pltpu.VMEM((ROWS, NY), F32),
            pltpu.VMEM((64, NZ), F32),
            pltpu.VMEM((64, NZ), F32),
            pltpu.SMEM((LABELS,), F32),
            pltpu.SMEM((LABELS,), F32),
            pltpu.VMEM(field, F32),
            pltpu.VMEM((3,) + field, F32),
            pltpu.VMEM(field, jnp.int32),
            pltpu.VMEM((SRC // NY, NY), jnp.int32),
            pltpu.VMEM((SRC // NY, NY), F32),
            pltpu.VMEM((4, NX, NX), BF16),
            pltpu.VMEM((4, NZ, NZ), BF16),
            pltpu.VMEM((3, ROWS, NY), F32),
            pltpu.VMEM((3, ROWS, NY), F32),
            pltpu.VMEM((ROWS, NY), F32),
            pltpu.VMEM((ROWS, NY), F32),
            pltpu.VMEM((64, NZ), F32),
            pltpu.VMEM((SRC // NY, NY), jnp.int32),
            pltpu.VMEM((SRC // NY, NY), jnp.int32),
            pltpu.SemaphoreType.DMA((14,)),
            pltpu.SemaphoreType.DMA((14,)),
            pltpu.SemaphoreType.DMA((9,)),
        ],
        compiler_params=pltpu.CompilerParams(collective_id=0, has_side_effects=True),
    )(
        sound_table,
        mass_table,
        density,
        velocity,
        labels,
        source_index.reshape(SRC // NY, NY),
        source_values[0].reshape(SRC // NY, NY),
        jnp.asarray(small),
        jnp.asarray(large),
    )


def solution(mesh):
    in_specs = (
        P("gz", "gx", None),
        P(None, "gz", "gx", None),
        P("gz", "gx", None),
        P(),
        P(),
        P(),
        P(),
    )
    out_specs = (P("gz", "gx", None), P(None, "gz", "gx", None))
    return jax.shard_map(shards, mesh=mesh, in_specs=in_specs, out_specs=out_specs, check_vma=False)
```

```python
import math

import jax
import jax.numpy as jnp
import numpy as np
from jax import lax
from jax.experimental import pallas as pl
from jax.experimental.pallas import tpu as pltpu
from jax.sharding import PartitionSpec as P

NZ = 512
NX = 128
NY = 128
LABELS = 8
PML_W = 20
SRC = 4096
DT = 0.3
ABSORB = 2.0
CHIPS = 128
WIDE = CHIPS * 8
Z_LOC = 8
X_LOC = 32
ROWS = Z_LOC * X_LOC
MESH = pl.DeviceIdType.MESH
F32 = jnp.float32
BF16 = jnp.bfloat16

P_S, U0_S, UX_S, UZ_S, VY_S, VX_S, VZ_S, E_S = range(8)
P_C, X_C, YZ_C = range(3)
V0_I, VX_I, E_I = range(3)


def basis(n):
    j = np.arange(n)
    f = np.concatenate([np.arange(n // 2 + 1), np.arange(1, n // 2)])
    is_sin = (np.arange(n) > n // 2)[:, None]
    scale = np.where((f == 0) | (f == n // 2), math.sqrt(1.0 / n), math.sqrt(2.0 / n))[:, None]
    k = (2.0 * math.pi / n * f)[:, None]
    phase = 2.0 * math.pi / n * ((f[:, None] * j[None, :]) % n)
    half = 2.0 * math.pi / (2 * n) * ((f[:, None] * (2 * j[None, :] + 1)) % (2 * n))
    forward = np.where(is_sin, np.sin(phase), np.cos(phase)) * scale
    slope = np.where(is_sin, k * np.cos(half), -k * np.sin(half)) * scale
    return forward, slope


def parts(table):
    table = table.astype(np.float32)
    high = table.astype(jnp.bfloat16)
    low = (table - high.astype(np.float32)).astype(jnp.bfloat16)
    return [high, low]


def tables():
    r, d = basis(NX)
    lane = np.arange(NX)
    x_of = [((lane % 64) // 32 * 2 + (lane // 64 + core) % 2) * X_LOC + lane % 32 for core in range(2)]
    small = np.stack([np.stack(parts(r[:, x]) + parts(d[:, x])) for x in [lane] + x_of])
    r, d = basis(NZ)
    row = np.arange(NZ)
    z = (row % 64) * Z_LOC + row // 64
    large = np.stack(parts(r[:, z]) + parts(d[:, z]))
    return small, large


def split(x):
    high = x.astype(BF16)
    return high, (x - high.astype(F32)).astype(BF16)


def product(a, b, dims):
    contract = (((1,), (0 if dims == "nn" else 1,)), ((), ()))
    a, b = (x() if callable(x) else x for x in (a, b))

    def dot(u, v):
        return lax.dot_general(u, v, contract, preferred_element_type=F32)

    return dot(a[0], b[0]) + dot(a[1], b[0]) + dot(a[0], b[1])


def interleave(u, v):
    even = lax.broadcasted_iota(jnp.int32, u.shape, 1) % 64 < 32
    return jnp.where(even, u, pltpu.roll(v, 32, 1)), jnp.where(even, pltpu.roll(u, 96, 1), v)


def low_half(shape):
    return lax.broadcasted_iota(jnp.int32, shape, 1) < 64


def both(u):
    low = low_half(u.shape)
    other = pltpu.roll(u, 64, 1)
    return jnp.where(low, u, other), jnp.where(low, other, u)


def kernel(
    sound_hbm, mass_hbm, dens_hbm, vel_hbm, lab_hbm, sidx_hbm, sval_hbm, small_hbm, large_hbm,
    out_d, out_v,
    send_buf, recv_buf, half_send, half_recv, back_send, back_recv,
    sound, mass, dens, vel, lab, sidx, sval, flat, mixed, large, turned_large,
    base_v, coef_v, base_d, coef_d, corr, row_of, col_of,
    send_sem, recv_sem, half_sem, half_got, back_sem, back_got, load_sem,
):
    gz = lax.axis_index("gz")
    gx = lax.axis_index("gx")
    core = lax.rem(gx, 2)
    me = gz * 2 + lax.div(gx, 2)
    partner = (gz, gx + 1 - 2 * core)

    loads = [
        pltpu.make_async_copy(away, here, load_sem.at[i])
        for i, (away, here) in enumerate(
            (
                (sound_hbm, sound),
                (lab_hbm, lab),
                (dens_hbm, dens),
                (small_hbm.at[0], flat),
                (mass_hbm, mass),
                (vel_hbm, vel),
                (sidx_hbm, sidx),
                (sval_hbm, sval),
                (small_hbm.at[1 + core], mixed),
                (large_hbm, large),
            )
        )
    ]
    for load in loads:
        load.start()

    own_low = lax.div(gx, 2)
    neighbour = (gz, gx + 2 - 4 * own_low)

    def each_peer(visit):
        def place(at, carry):
            for low in range(2):
                visit(at, low, (at, 2 * low + core))
            return carry

        def pair(step, carry):
            place(lax.rem(gz + 32 + step, 64), 0)
            place(lax.rem(gz + 32 - step, 64), 0)
            return carry

        place(lax.rem(gz + 32, 64), 0)
        lax.fori_loop(1, 32, pair, 0)
        visit(gz, 1 - own_low, neighbour)

    barrier = pltpu.get_barrier_semaphore()

    def greet(at, low, device):
        pl.semaphore_signal(barrier, inc=1, device_id=device, device_id_type=MESH)

    each_peer(greet)
    pl.semaphore_signal(barrier, inc=1, device_id=partner, device_id_type=MESH)

    def send(which):
        own = pl.ds(pl.multiple_of(me * 8, 8), 2)
        recv_buf[which, own, :] = send_buf[which, own, :]

        def one(at, low, device):
            pltpu.make_async_remote_copy(
                send_buf.at[which, pl.ds(pl.multiple_of(at * 16 + low * 8, 8), 2)],
                recv_buf.at[which, own],
                send_sem.at[which],
                recv_sem.at[which],
                device_id=device,
                device_id_type=MESH,
            ).start()

        each_peer(one)

    some = pl.ds(0, 2 * (CHIPS - 1))

    def arrived(which):
        pltpu.make_async_copy(
            send_buf.at[which, some], recv_buf.at[which, some], recv_sem.at[which]
        ).wait()

    def sent(which):
        pltpu.make_async_copy(
            send_buf.at[which, some], recv_buf.at[which, some], send_sem.at[which]
        ).wait()

    def put(which, value):
        for tile in range(2):
            send_buf[which, pl.ds(tile, CHIPS, stride=8), :] = value[:, tile * 128 : tile * 128 + 128]

    def turned(which):
        tiles = [recv_buf[which, pl.ds(tile, CHIPS, stride=8), :].T for tile in range(2)]
        return split(jnp.concatenate(tiles, axis=0))

    def get_slab(which):
        blocks = []
        for tile in range(2):
            near = [recv_buf[which, pl.ds(tile + 8 * low, 64, stride=16), :] for low in range(2)]
            b0, b1 = interleave(*near)
            q0, q2 = both(b0)
            q1, q3 = both(b1)
            blocks += [q0, q1, q2, q3]
        return split(jnp.concatenate(blocks, axis=0))

    def put_slab(which, value):
        low = low_half((64, 128))
        for tile in range(2):
            q = [value[(tile * 4 + i) * 64 : (tile * 4 + i) * 64 + 64] for i in range(4)]
            near = interleave(jnp.where(low, q[0], q[2]), jnp.where(low, q[1], q[3]))
            for at in range(2):
                send_buf[which, pl.ds(tile + 8 * at, 64, stride=16), :] = near[at]

    low = low_half((128, 128))

    def give_half(which, value):
        for half in range(2):
            top = value[half * 256 : half * 256 + 128]
            bottom = value[half * 256 + 128 : half * 256 + 256]
            half_send[which, half] = jnp.where(low, top, bottom)
        copy = pltpu.make_async_remote_copy(
            half_send.at[which, 1 - core],
            half_recv.at[which],
            half_sem.at[which],
            half_got.at[which],
            device_id=partner,
            device_id_type=MESH,
        )
        copy.start()
        return copy

    def take_half(which, copy):
        copy.wait_recv()
        mine = half_send[which, core]
        other = half_recv[which]
        top = jnp.where(low, mine, pltpu.roll(other, 64, 1))
        bottom = jnp.where(low, pltpu.roll(mine, 64, 1), other)
        return split(jnp.concatenate([top, bottom], axis=0))

    def give_back(which, value):
        top, bottom = value[:128], value[128:]
        back_recv[which, core] = jnp.where(low, top, pltpu.roll(bottom, 64, 1))
        back_send[which] = jnp.where(low, pltpu.roll(top, 64, 1), bottom)
        copy = pltpu.make_async_remote_copy(
            back_send.at[which],
            back_recv.at[which, core],
            back_sem.at[which],
            back_got.at[which],
            device_id=partner,
            device_id_type=MESH,
        )
        copy.start()
        return copy

    def take_back(which, copy):
        copy.wait_recv()
        return split(jnp.concatenate(both(back_recv[which, 0]) + both(back_recv[which, 1]), axis=0))

    for load in loads[:4]:
        load.wait()
    def r_flat():
        return flat[0], flat[1]

    def d_flat():
        return flat[2], flat[3]

    speed_ref = sound[0]
    for tissue in range(1, LABELS):
        speed_ref = jnp.maximum(speed_ref, sound[tissue])

    classes = lab[...].reshape(ROWS, NY)
    speed = jnp.full((ROWS, NY), sound[0])
    for tissue in range(1, LABELS):
        speed = jnp.where(classes == tissue, sound[tissue], speed)
    pressure = speed * speed * dens[...].reshape(ROWS, NY)
    put(P_S, product(r_flat, split(pressure), "nt"))
    pl.semaphore_wait(barrier, CHIPS)
    send(P_S)

    for load in loads[4:8]:
        load.wait()
    density_mass = jnp.full((ROWS, NY), mass[0])
    for tissue in range(1, LABELS):
        density_mass = jnp.where(classes == tissue, mass[tissue], density_mass)
    row = lax.broadcasted_iota(jnp.int32, (ROWS, NY), 0)
    col = lax.broadcasted_iota(jnp.int32, (ROWS, NY), 1)

    def damping(position, length):
        coordinate = position.astype(F32)
        depth = jnp.maximum(
            jnp.maximum(PML_W - coordinate, coordinate - (length - 1 - PML_W)), 0.0
        ) / PML_W
        square = depth * depth
        return jnp.exp(-ABSORB * speed_ref * (square * square) * DT * 0.5)

    damp = (
        damping(gz * Z_LOC + row // X_LOC, NZ),
        damping(gx * X_LOC + row % X_LOC, NX),
        damping(col, NY),
    )
    over_mass = DT / density_mass
    for a in range(3):
        base_v[a] = damp[a] * (damp[a] * vel[a].reshape(ROWS, NY))
        coef_v[a] = damp[a] * over_mass
    damp_all = damp[0] * damp[1] * damp[2]
    base_d[...] = damp_all * (damp_all * dens[...].reshape(ROWS, NY))
    coef_d[...] = damp_all * (DT * density_mass)

    line = lax.broadcasted_iota(jnp.int32, (256, NX), 0)
    index_x = lax.broadcasted_iota(jnp.int32, (256, NX), 1)

    def wave(index, length):
        folded = jnp.where(index <= length // 2, index, index - length // 2)
        return folded.astype(F32) * (2.0 * math.pi / length)

    wz = wave(core * 256 + line, NZ)
    wx = wave(index_x, NX)
    wy = wave(jnp.full((256, NX), me, jnp.int32), NY)
    angle = speed_ref * jnp.sqrt(wz * wz + wx * wx + wy * wy) * (DT / 2.0)
    at_zero = angle == 0.0
    safe = jnp.where(at_zero, 1.0, angle)
    corr[...] = jnp.where(at_zero, 1.0, jnp.sin(safe) / safe)

    for load in loads[8:]:
        load.wait()
    for table in range(4):
        turned_large[table] = large[table].T
    def r_mixed():
        return mixed[0], mixed[1]

    def d_mixed():
        return mixed[2], mixed[3]

    def r_large():
        return large[0], large[1]

    def d_large():
        return large[2], large[3]

    def r_turned():
        return turned_large[0], turned_large[1]

    def d_turned():
        return turned_large[2], turned_large[3]

    copies = []

    arrived(P_S)
    copy = give_half(P_C, product(r_large, get_slab(P_S), "nn"))
    copies.append(copy)
    spectrum = product(take_half(P_C, copy), r_mixed, "nt")
    spectrum = split(spectrum * corr[...])
    back_0 = give_back(V0_I, product(spectrum, r_mixed, "nn"))
    back_x = give_back(VX_I, product(spectrum, d_mixed, "nn"))
    copies += [back_0, back_x]
    field = take_back(V0_I, back_0)
    put_slab(U0_S, product(r_turned, field, "nn"))
    send(U0_S)
    put_slab(UX_S, product(r_turned, take_back(VX_I, back_x), "nn"))
    send(UX_S)
    put_slab(UZ_S, product(d_turned, field, "nn"))
    send(UZ_S)

    where = sidx[...]
    plane = NX * NY
    z_off = where // plane - gz * Z_LOC
    remain = where % plane
    x_off = remain // NY - gx * X_LOC
    inside = (z_off >= 0) & (z_off < Z_LOC) & (x_off >= 0) & (x_off < X_LOC)
    row_of[...] = jnp.where(inside, z_off * X_LOC + x_off, -1)
    col_of[...] = remain % NY

    def add_some(step, carry):
        picks = []
        highs = []
        lows = []
        for part in range(2):
            at = pl.ds(step * 2 + part, 1)
            picks.append(jnp.where(row == row_of[at, :], 1.0, 0.0).astype(BF16))
            amount = jnp.where(row[:NY] == col_of[at, :], sval[at, :], 0.0)
            high, low = split(amount)
            highs.append(high)
            lows.append(low)
        pick = jnp.concatenate(picks, axis=1)
        contract = (((1,), (1,)), ((), ()))
        high = lax.dot_general(pick, jnp.concatenate(highs, axis=1), contract, preferred_element_type=F32)
        low = lax.dot_general(pick, jnp.concatenate(lows, axis=1), contract, preferred_element_type=F32)
        base_d[...] += high + low
        return carry

    lax.fori_loop(0, SRC // NY // 2, add_some, 0)

    for came, goes, a, back, sign in (
        (U0_S, VY_S, 2, d_flat, -1),
        (UX_S, VX_S, 1, r_flat, 1),
        (UZ_S, VZ_S, 0, r_flat, 1),
    ):
        arrived(came)
        slope = product(turned(came), back, "nn")
        fresh = base_v[a] - coef_v[a] * slope
        halves = split(fresh)
        if sign > 0:
            put(goes, product(r_flat, halves, "nt"))
        else:
            put(goes, -product(d_flat, halves, "nt"))
        send(goes)
        out_v[a] = fresh.reshape(Z_LOC, X_LOC, NY)

    arrived(VY_S)
    part_yz = product(r_large, get_slab(VY_S), "nn")
    arrived(VX_S)
    copy_x = give_half(X_C, product(r_large, get_slab(VX_S), "nn"))
    spectrum = product(take_half(X_C, copy_x), d_mixed, "nt")
    arrived(VZ_S)
    copy_yz = give_half(YZ_C, part_yz - product(d_large, get_slab(VZ_S), "nn"))
    spectrum = product(take_half(YZ_C, copy_yz), r_mixed, "nt") - spectrum
    back_e = give_back(E_I, product(split(spectrum * corr[...]), r_mixed, "nn"))
    copies += [copy_x, copy_yz, back_e]
    put_slab(E_S, product(r_turned, take_back(E_I, back_e), "nn"))
    send(E_S)

    arrived(E_S)
    spread = product(turned(E_S), r_flat, "nn")
    out_d[...] = (base_d[...] - coef_d[...] * spread).reshape(Z_LOC, X_LOC, NY)
    for which in range(8):
        sent(which)
    for copy in copies:
        copy.wait_send()


def shards(density, velocity, labels, sound_table, mass_table, source_index, source_values):
    small, large = tables()
    vmem = pl.BlockSpec(memory_space=pltpu.VMEM)
    hbm = pl.BlockSpec(memory_space=pl.ANY)
    field = (Z_LOC, X_LOC, NY)
    return pl.pallas_call(
        kernel,
        out_shape=(
            pltpu.VMEM(field, F32),
            pltpu.VMEM((3,) + field, F32),
        ),
        in_specs=[hbm] * 9,
        out_specs=(vmem, vmem),
        scratch_shapes=[
            pltpu.VMEM((8, WIDE, 128), F32),
            pltpu.VMEM((8, WIDE, 128), F32),
            pltpu.VMEM((3, 2, 128, 128), F32),
            pltpu.VMEM((3, 128, 128), F32),
            pltpu.VMEM((3, 128, 128), F32),
            pltpu.VMEM((3, 2, 128, 128), F32),
            pltpu.SMEM((LABELS,), F32),
            pltpu.SMEM((LABELS,), F32),
            pltpu.VMEM(field, F32),
            pltpu.VMEM((3,) + field, F32),
            pltpu.VMEM(field, jnp.int32),
            pltpu.VMEM((SRC // NY, NY), jnp.int32),
            pltpu.VMEM((SRC // NY, NY), F32),
            pltpu.VMEM((4, NX, NX), BF16),
            pltpu.VMEM((4, NX, NX), BF16),
            pltpu.VMEM((4, NZ, NZ), BF16),
            pltpu.VMEM((4, NZ, NZ), BF16),
            pltpu.VMEM((3, ROWS, NY), F32),
            pltpu.VMEM((3, ROWS, NY), F32),
            pltpu.VMEM((ROWS, NY), F32),
            pltpu.VMEM((ROWS, NY), F32),
            pltpu.VMEM((256, NX), F32),
            pltpu.VMEM((SRC // NY, NY), jnp.int32),
            pltpu.VMEM((SRC // NY, NY), jnp.int32),
            pltpu.SemaphoreType.DMA((8,)),
            pltpu.SemaphoreType.DMA((8,)),
            pltpu.SemaphoreType.DMA((3,)),
            pltpu.SemaphoreType.DMA((3,)),
            pltpu.SemaphoreType.DMA((3,)),
            pltpu.SemaphoreType.DMA((3,)),
            pltpu.SemaphoreType.DMA((10,)),
        ],
        compiler_params=pltpu.CompilerParams(collective_id=0, has_side_effects=True),
    )(
        sound_table,
        mass_table,
        density,
        velocity,
        labels,
        source_index.reshape(SRC // NY, NY),
        source_values[0].reshape(SRC // NY, NY),
        jnp.asarray(small),
        jnp.asarray(large),
    )


def solution(mesh):
    in_specs = (
        P("gz", "gx", None),
        P(None, "gz", "gx", None),
        P("gz", "gx", None),
        P(),
        P(),
        P(),
        P(),
    )
    out_specs = (P("gz", "gx", None), P(None, "gz", "gx", None))
    return jax.shard_map(shards, mesh=mesh, in_specs=in_specs, out_specs=out_specs, check_vma=False)
```

```python
import math

import jax
import jax.numpy as jnp
import numpy as np
from jax import lax
from jax.experimental import pallas as pl
from jax.experimental.pallas import tpu as pltpu
from jax.sharding import PartitionSpec as P

NZ = 512
NX = 128
NY = 128
LABELS = 8
PML_W = 20
SRC = 4096
DT = 0.3
ABSORB = 2.0
CHIPS = 128
WIDE = CHIPS * 8
Z_LOC = 8
X_LOC = 32
ROWS = Z_LOC * X_LOC
MESH = pl.DeviceIdType.MESH
F32 = jnp.float32
BF16 = jnp.bfloat16

P_S, U0_S, UX_S, UZ_S, VY_S, VX_S, VZ_S, E_S = range(8)
P_C, X_C, YZ_C = range(3)
V0_I, VX_I, E_I = range(3)


def basis(n):
    j = np.arange(n)
    f = np.concatenate([np.arange(n // 2 + 1), np.arange(1, n // 2)])
    is_sin = (np.arange(n) > n // 2)[:, None]
    scale = np.where((f == 0) | (f == n // 2), math.sqrt(1.0 / n), math.sqrt(2.0 / n))[:, None]
    k = (2.0 * math.pi / n * f)[:, None]
    phase = 2.0 * math.pi / n * ((f[:, None] * j[None, :]) % n)
    half = 2.0 * math.pi / (2 * n) * ((f[:, None] * (2 * j[None, :] + 1)) % (2 * n))
    forward = np.where(is_sin, np.sin(phase), np.cos(phase)) * scale
    slope = np.where(is_sin, k * np.cos(half), -k * np.sin(half)) * scale
    return forward, slope


def parts(table):
    table = table.astype(np.float32)
    high = table.astype(jnp.bfloat16)
    low = (table - high.astype(np.float32)).astype(jnp.bfloat16)
    return [high, low]


def tables():
    r, d = basis(NX)
    lane = np.arange(NX)
    x_of = [((lane % 64) // 32 * 2 + (lane // 64 + core) % 2) * X_LOC + lane % 32 for core in range(2)]
    small = np.stack([np.stack(parts(r[:, x]) + parts(d[:, x])) for x in [lane] + x_of])
    r, d = basis(NZ)
    frequency = np.concatenate([np.arange(NZ // 2 + 1), np.arange(1, NZ // 2)])
    row = np.arange(NZ // 2)
    z = (row % 32) * Z_LOC + row // 32
    large = np.stack(
        [
            np.stack(parts(r[frequency % 2 == odd][:, z]) + parts(d[frequency % 2 == odd][:, z]))
            for odd in range(2)
        ]
    )
    return small, large


def split(x):
    high = x.astype(BF16)
    return high, (x - high.astype(F32)).astype(BF16)


def product(a, b, dims):
    contract = (((1,), (0 if dims == "nn" else 1,)), ((), ()))
    a, b = (x() if callable(x) else x for x in (a, b))

    def dot(u, v):
        return lax.dot_general(u, v, contract, preferred_element_type=F32)

    return dot(a[0], b[0]) + dot(a[1], b[0]) + dot(a[0], b[1])


def interleave(u, v):
    even = lax.broadcasted_iota(jnp.int32, u.shape, 1) % 64 < 32
    return jnp.where(even, u, pltpu.roll(v, 32, 1)), jnp.where(even, pltpu.roll(u, 96, 1), v)


def low_half(shape):
    return lax.broadcasted_iota(jnp.int32, shape, 1) < 64


def both(u):
    low = low_half(u.shape)
    other = pltpu.roll(u, 64, 1)
    return jnp.where(low, u, other), jnp.where(low, other, u)


def kernel(
    sound_hbm, mass_hbm, dens_hbm, vel_hbm, lab_hbm, sidx_hbm, sval_hbm, small_hbm, large_hbm,
    out_d, out_v,
    send_buf, recv_buf, half_send, half_recv, back_send, back_recv,
    sound, mass, dens, vel, lab, sidx, sval, flat, mixed, large, turned_large,
    base_v, coef_v, base_d, coef_d, corr, row_of, col_of,
    send_sem, recv_sem, half_sem, half_got, back_sem, back_got, load_sem,
):
    gz = lax.axis_index("gz")
    gx = lax.axis_index("gx")
    core = lax.rem(gx, 2)
    me = gz * 2 + lax.div(gx, 2)
    partner = (gz, gx + 1 - 2 * core)

    loads = [
        pltpu.make_async_copy(away, here, load_sem.at[i])
        for i, (away, here) in enumerate(
            (
                (sound_hbm, sound),
                (lab_hbm, lab),
                (dens_hbm, dens),
                (small_hbm.at[0], flat),
                (mass_hbm, mass),
                (vel_hbm, vel),
                (sidx_hbm, sidx),
                (sval_hbm, sval),
                (small_hbm.at[1 + core], mixed),
                (large_hbm, large),
            )
        )
    ]
    for load in loads:
        load.start()

    own_low = lax.div(gx, 2)
    neighbour = (gz, gx + 2 - 4 * own_low)

    def each_peer(visit):
        def place(at, carry):
            for low in range(2):
                visit(at, low, (at, 2 * low + core))
            return carry

        def pair(step, carry):
            place(lax.rem(gz + 32 + step, 64), 0)
            place(lax.rem(gz + 32 - step, 64), 0)
            return carry

        place(lax.rem(gz + 32, 64), 0)
        lax.fori_loop(1, 32, pair, 0)
        visit(gz, 1 - own_low, neighbour)

    barrier = pltpu.get_barrier_semaphore()

    def greet(at, low, device):
        pl.semaphore_signal(barrier, inc=1, device_id=device, device_id_type=MESH)

    each_peer(greet)
    pl.semaphore_signal(barrier, inc=1, device_id=partner, device_id_type=MESH)

    def send(which):
        own = pl.ds(pl.multiple_of(me * 8, 8), 2)
        recv_buf[which, own, :] = send_buf[which, own, :]

        def one(at, low, device):
            pltpu.make_async_remote_copy(
                send_buf.at[which, pl.ds(pl.multiple_of(at * 16 + low * 8, 8), 2)],
                recv_buf.at[which, own],
                send_sem.at[which],
                recv_sem.at[which],
                device_id=device,
                device_id_type=MESH,
            ).start()

        each_peer(one)

    some = pl.ds(0, 2 * (CHIPS - 1))

    def arrived(which):
        pltpu.make_async_copy(
            send_buf.at[which, some], recv_buf.at[which, some], recv_sem.at[which]
        ).wait()

    def sent(which):
        pltpu.make_async_copy(
            send_buf.at[which, some], recv_buf.at[which, some], send_sem.at[which]
        ).wait()

    def put(which, value):
        for tile in range(2):
            send_buf[which, pl.ds(tile, CHIPS, stride=8), :] = value[:, tile * 128 : tile * 128 + 128]

    def turned(which):
        tiles = [recv_buf[which, pl.ds(tile, CHIPS, stride=8), :].T for tile in range(2)]
        return split(jnp.concatenate(tiles, axis=0))

    low = low_half((128, 128))
    low_32 = low_half((32, 128))

    def stacked(blocks):
        value = jnp.concatenate(blocks, axis=0)
        high = value.astype(BF16).astype(F32)
        return jnp.where(low_half(value.shape), value, value - high).astype(BF16)

    def long_product(tables, value):
        def dot(table):
            return jnp.dot(table, value, preferred_element_type=F32)

        return dot(tables[0]) + dot(tables[1])

    def combine(u, v, mask):
        return jnp.where(mask, u, v) + pltpu.roll(jnp.where(mask, v, u), 64, 1)

    def get_slab(which):
        folds = ([], [])
        for tile in range(2):
            near = [recv_buf[which, pl.ds(tile + 8 * at, 64, stride=16), :] for at in range(2)]
            for blocks, sign in zip(folds, (1, -1)):
                b0, b1 = interleave(*[a[:32] + sign * a[32:] for a in near])
                q0, q2 = both(b0)
                q1, q3 = both(b1)
                blocks += [q0, q1, q2, q3]
        return [stacked(blocks) for blocks in folds]

    def put_slab(which, folds):
        for tile in range(2):
            ends = []
            for value in folds:
                q = [value[(tile * 4 + i) * 32 : (tile * 4 + i) * 32 + 32] for i in range(4)]
                ends.append(interleave(combine(q[0], q[2], low_32), combine(q[1], q[3], low_32)))
            for at in range(2):
                first = tile + 8 * at
                send_buf[which, pl.ds(first, 32, stride=16), :] = ends[0][at] + ends[1][at]
                send_buf[which, pl.ds(first + 512, 32, stride=16), :] = ends[0][at] - ends[1][at]

    def along_z(table, folds):
        return [long_product((table[h, 0], table[h, 1]), folds[h]) for h in range(2)]


    def give_half(which, value):
        for half in range(2):
            half_send[which, half] = combine(value[half][:128], value[half][128:], low)
        copy = pltpu.make_async_remote_copy(
            half_send.at[which, 1 - core],
            half_recv.at[which],
            half_sem.at[which],
            half_got.at[which],
            device_id=partner,
            device_id_type=MESH,
        )
        copy.start()
        return copy

    def take_half(which, copy):
        copy.wait_recv()
        mine = half_send[which, core]
        other = half_recv[which]
        top = jnp.where(low, mine, pltpu.roll(other, 64, 1))
        bottom = jnp.where(low, pltpu.roll(mine, 64, 1), other)
        return split(jnp.concatenate([top, bottom], axis=0))

    def give_back(which, value):
        top, bottom = value[:128], value[128:]
        back_recv[which, core] = jnp.where(low, top, pltpu.roll(bottom, 64, 1))
        back_send[which] = jnp.where(low, pltpu.roll(top, 64, 1), bottom)
        copy = pltpu.make_async_remote_copy(
            back_send.at[which],
            back_recv.at[which, core],
            back_sem.at[which],
            back_got.at[which],
            device_id=partner,
            device_id_type=MESH,
        )
        copy.start()
        return copy

    def take_back(which, copy):
        copy.wait_recv()
        return [stacked(both(back_recv[which, half])) for half in range(2)]

    for load in loads[:4]:
        load.wait()
    def r_flat():
        return flat[0], flat[1]

    def d_flat():
        return flat[2], flat[3]

    speed_ref = sound[0]
    for tissue in range(1, LABELS):
        speed_ref = jnp.maximum(speed_ref, sound[tissue])

    classes = lab[...].reshape(ROWS, NY)
    speed = jnp.full((ROWS, NY), sound[0])
    for tissue in range(1, LABELS):
        speed = jnp.where(classes == tissue, sound[tissue], speed)
    pressure = speed * speed * dens[...].reshape(ROWS, NY)
    put(P_S, product(r_flat, split(pressure), "nt"))
    pl.semaphore_wait(barrier, CHIPS)
    send(P_S)

    for load in loads[4:8]:
        load.wait()
    density_mass = jnp.full((ROWS, NY), mass[0])
    for tissue in range(1, LABELS):
        density_mass = jnp.where(classes == tissue, mass[tissue], density_mass)
    row = lax.broadcasted_iota(jnp.int32, (ROWS, NY), 0)
    col = lax.broadcasted_iota(jnp.int32, (ROWS, NY), 1)

    def damping(position, length):
        coordinate = position.astype(F32)
        depth = jnp.maximum(
            jnp.maximum(PML_W - coordinate, coordinate - (length - 1 - PML_W)), 0.0
        ) / PML_W
        square = depth * depth
        return jnp.exp(-ABSORB * speed_ref * (square * square) * DT * 0.5)

    damp = (
        damping(gz * Z_LOC + row // X_LOC, NZ),
        damping(gx * X_LOC + row % X_LOC, NX),
        damping(col, NY),
    )
    over_mass = DT / density_mass
    for a in range(3):
        base_v[a] = damp[a] * (damp[a] * vel[a].reshape(ROWS, NY))
        coef_v[a] = damp[a] * over_mass
    damp_all = damp[0] * damp[1] * damp[2]
    base_d[...] = damp_all * (damp_all * dens[...].reshape(ROWS, NY))
    coef_d[...] = damp_all * (DT * density_mass)

    line = lax.broadcasted_iota(jnp.int32, (256, NX), 0)
    index_x = lax.broadcasted_iota(jnp.int32, (256, NX), 1)

    def wave(index, length):
        folded = jnp.where(index <= length // 2, index, index - length // 2)
        return folded.astype(F32) * (2.0 * math.pi / length)

    folded = jnp.where(line <= 128 - core, line, line - 128)
    wz = (2 * folded + core).astype(F32) * (2.0 * math.pi / NZ)
    wx = wave(index_x, NX)
    wy = wave(jnp.full((256, NX), me, jnp.int32), NY)
    angle = speed_ref * jnp.sqrt(wz * wz + wx * wx + wy * wy) * (DT / 2.0)
    at_zero = angle == 0.0
    safe = jnp.where(at_zero, 1.0, angle)
    corr[...] = jnp.where(at_zero, 1.0, jnp.sin(safe) / safe)

    for load in loads[8:]:
        load.wait()
    for half in range(2):
        for table in range(4):
            turned_large[half, table] = large[half, table].T
    r_large, d_large = large.at[:, 0:2], large.at[:, 2:4]
    r_turned, d_turned = turned_large.at[:, 0:2], turned_large.at[:, 2:4]

    def r_mixed():
        return mixed[0], mixed[1]

    def d_mixed():
        return mixed[2], mixed[3]

    copies = []

    arrived(P_S)
    copy = give_half(P_C, along_z(r_large, get_slab(P_S)))
    copies.append(copy)
    spectrum = product(take_half(P_C, copy), r_mixed, "nt")
    spectrum = split(spectrum * corr[...])
    back_0 = give_back(V0_I, product(spectrum, r_mixed, "nn"))
    back_x = give_back(VX_I, product(spectrum, d_mixed, "nn"))
    copies += [back_0, back_x]
    field = take_back(V0_I, back_0)
    put_slab(U0_S, along_z(r_turned, field))
    send(U0_S)
    put_slab(UX_S, along_z(r_turned, take_back(VX_I, back_x)))
    send(UX_S)
    put_slab(UZ_S, along_z(d_turned, field))
    send(UZ_S)

    where = sidx[...]
    plane = NX * NY
    z_off = where // plane - gz * Z_LOC
    remain = where % plane
    x_off = remain // NY - gx * X_LOC
    inside = (z_off >= 0) & (z_off < Z_LOC) & (x_off >= 0) & (x_off < X_LOC)
    row_of[...] = jnp.where(inside, z_off * X_LOC + x_off, -1)
    col_of[...] = remain % NY

    def add_some(step, carry):
        picks = []
        highs = []
        lows = []
        for part in range(2):
            at = pl.ds(step * 2 + part, 1)
            picks.append(jnp.where(row == row_of[at, :], 1.0, 0.0).astype(BF16))
            amount = jnp.where(row[:NY] == col_of[at, :], sval[at, :], 0.0)
            high, low = split(amount)
            highs.append(high)
            lows.append(low)
        pick = jnp.concatenate(picks, axis=1)
        contract = (((1,), (1,)), ((), ()))
        high = lax.dot_general(pick, jnp.concatenate(highs, axis=1), contract, preferred_element_type=F32)
        low = lax.dot_general(pick, jnp.concatenate(lows, axis=1), contract, preferred_element_type=F32)
        base_d[...] += high + low
        return carry

    lax.fori_loop(0, SRC // NY // 2, add_some, 0)

    for came, goes, a, back, sign in (
        (U0_S, VY_S, 2, d_flat, -1),
        (UX_S, VX_S, 1, r_flat, 1),
        (UZ_S, VZ_S, 0, r_flat, 1),
    ):
        arrived(came)
        slope = product(turned(came), back, "nn")
        fresh = base_v[a] - coef_v[a] * slope
        halves = split(fresh)
        if sign > 0:
            put(goes, product(r_flat, halves, "nt"))
        else:
            put(goes, -product(d_flat, halves, "nt"))
        send(goes)
        out_v[a] = fresh.reshape(Z_LOC, X_LOC, NY)

    arrived(VY_S)
    part_yz = along_z(r_large, get_slab(VY_S))
    arrived(VX_S)
    copy_x = give_half(X_C, along_z(r_large, get_slab(VX_S)))
    spectrum = product(take_half(X_C, copy_x), d_mixed, "nt")
    arrived(VZ_S)
    copy_yz = give_half(
        YZ_C, [y - z for y, z in zip(part_yz, along_z(d_large, get_slab(VZ_S)))]
    )
    spectrum = product(take_half(YZ_C, copy_yz), r_mixed, "nt") - spectrum
    back_e = give_back(E_I, product(split(spectrum * corr[...]), r_mixed, "nn"))
    copies += [copy_x, copy_yz, back_e]
    put_slab(E_S, along_z(r_turned, take_back(E_I, back_e)))
    send(E_S)

    arrived(E_S)
    spread = product(turned(E_S), r_flat, "nn")
    out_d[...] = (base_d[...] - coef_d[...] * spread).reshape(Z_LOC, X_LOC, NY)
    for which in range(8):
        sent(which)
    for copy in copies:
        copy.wait_send()


def shards(density, velocity, labels, sound_table, mass_table, source_index, source_values):
    small, large = tables()
    vmem = pl.BlockSpec(memory_space=pltpu.VMEM)
    hbm = pl.BlockSpec(memory_space=pl.ANY)
    field = (Z_LOC, X_LOC, NY)
    return pl.pallas_call(
        kernel,
        out_shape=(
            pltpu.VMEM(field, F32),
            pltpu.VMEM((3,) + field, F32),
        ),
        in_specs=[hbm] * 9,
        out_specs=(vmem, vmem),
        scratch_shapes=[
            pltpu.VMEM((8, WIDE, 128), F32),
            pltpu.VMEM((8, WIDE, 128), F32),
            pltpu.VMEM((3, 2, 128, 128), F32),
            pltpu.VMEM((3, 128, 128), F32),
            pltpu.VMEM((3, 128, 128), F32),
            pltpu.VMEM((3, 2, 128, 128), F32),
            pltpu.SMEM((LABELS,), F32),
            pltpu.SMEM((LABELS,), F32),
            pltpu.VMEM(field, F32),
            pltpu.VMEM((3,) + field, F32),
            pltpu.VMEM(field, jnp.int32),
            pltpu.VMEM((SRC // NY, NY), jnp.int32),
            pltpu.VMEM((SRC // NY, NY), F32),
            pltpu.VMEM((4, NX, NX), BF16),
            pltpu.VMEM((4, NX, NX), BF16),
            pltpu.VMEM((2, 4, NZ // 2, NZ // 2), BF16),
            pltpu.VMEM((2, 4, NZ // 2, NZ // 2), BF16),
            pltpu.VMEM((3, ROWS, NY), F32),
            pltpu.VMEM((3, ROWS, NY), F32),
            pltpu.VMEM((ROWS, NY), F32),
            pltpu.VMEM((ROWS, NY), F32),
            pltpu.VMEM((256, NX), F32),
            pltpu.VMEM((SRC // NY, NY), jnp.int32),
            pltpu.VMEM((SRC // NY, NY), jnp.int32),
            pltpu.SemaphoreType.DMA((8,)),
            pltpu.SemaphoreType.DMA((8,)),
            pltpu.SemaphoreType.DMA((3,)),
            pltpu.SemaphoreType.DMA((3,)),
            pltpu.SemaphoreType.DMA((3,)),
            pltpu.SemaphoreType.DMA((3,)),
            pltpu.SemaphoreType.DMA((10,)),
        ],
        compiler_params=pltpu.CompilerParams(collective_id=0, has_side_effects=True),
    )(
        sound_table,
        mass_table,
        density,
        velocity,
        labels,
        source_index.reshape(SRC // NY, NY),
        source_values[0].reshape(SRC // NY, NY),
        jnp.asarray(small),
        jnp.asarray(large),
    )


def solution(mesh):
    in_specs = (
        P("gz", "gx", None),
        P(None, "gz", "gx", None),
        P("gz", "gx", None),
        P(),
        P(),
        P(),
        P(),
    )
    out_specs = (P("gz", "gx", None), P(None, "gz", "gx", None))
    return jax.shard_map(shards, mesh=mesh, in_specs=in_specs, out_specs=out_specs, check_vma=False)
```

```python
import math

import jax
import jax.numpy as jnp
import numpy as np
from jax import lax
from jax.experimental import pallas as pl
from jax.experimental.pallas import tpu as pltpu
from jax.sharding import PartitionSpec as P

NZ = 512
NX = 128
NY = 128
LABELS = 8
PML_W = 20
SRC = 4096
DT = 0.3
ABSORB = 2.0
CHIPS = 128
WIDE = CHIPS * 8
Z_LOC = 8
X_LOC = 32
ROWS = Z_LOC * X_LOC
MESH = pl.DeviceIdType.MESH
F32 = jnp.float32
BF16 = jnp.bfloat16

P_S, U0_S, UX_S, UZ_S, VY_S, VX_S, VZ_S, E_S = range(8)
P_C, X_C, YZ_C = range(3)
V0_I, VX_I, E_I = range(3)


def basis(n):
    j = np.arange(n)
    f = np.concatenate([np.arange(n // 2 + 1), np.arange(1, n // 2)])
    is_sin = (np.arange(n) > n // 2)[:, None]
    scale = np.where((f == 0) | (f == n // 2), math.sqrt(1.0 / n), math.sqrt(2.0 / n))[:, None]
    k = (2.0 * math.pi / n * f)[:, None]
    phase = 2.0 * math.pi / n * ((f[:, None] * j[None, :]) % n)
    half = 2.0 * math.pi / (2 * n) * ((f[:, None] * (2 * j[None, :] + 1)) % (2 * n))
    forward = np.where(is_sin, np.sin(phase), np.cos(phase)) * scale
    slope = np.where(is_sin, k * np.cos(half), -k * np.sin(half)) * scale
    return forward, slope


def parts(table):
    table = table.astype(np.float32)
    high = table.astype(jnp.bfloat16)
    low = (table - high.astype(np.float32)).astype(jnp.bfloat16)
    return [high, low]


def tables():
    r, d = basis(NX)
    lane = np.arange(NX)
    x_of = [((lane % 64) // 32 * 2 + (lane // 64 + core) % 2) * X_LOC + lane % 32 for core in range(2)]
    small = np.stack([np.stack(parts(r[:, x]) + parts(d[:, x])) for x in [lane] + x_of])
    r, d = basis(NZ)
    frequency = np.concatenate([np.arange(NZ // 2 + 1), np.arange(1, NZ // 2)])
    row = np.arange(NZ // 2)
    z = (row % 32) * Z_LOC + row // 32
    large = np.stack(
        [
            np.stack(parts(r[frequency % 2 == odd][:, z]) + parts(d[frequency % 2 == odd][:, z]))
            for odd in range(2)
        ]
    )
    return small, large


def split(x):
    high = x.astype(BF16)
    return high, (x - high.astype(F32)).astype(BF16)


def product(a, b, dims):
    contract = (((1,), (0 if dims == "nn" else 1,)), ((), ()))
    a, b = (x() if callable(x) else x for x in (a, b))

    def dot(u, v):
        return lax.dot_general(u, v, contract, preferred_element_type=F32)

    return dot(a[0], b[0]) + dot(a[1], b[0]) + dot(a[0], b[1])


def interleave(u, v):
    even = lax.broadcasted_iota(jnp.int32, u.shape, 1) % 64 < 32
    return jnp.where(even, u, pltpu.roll(v, 32, 1)), jnp.where(even, pltpu.roll(u, 96, 1), v)


def low_half(shape):
    return lax.broadcasted_iota(jnp.int32, shape, 1) < 64


def both(u):
    low = low_half(u.shape)
    other = pltpu.roll(u, 64, 1)
    return jnp.where(low, u, other), jnp.where(low, other, u)


def kernel(
    sound_hbm, mass_hbm, dens_hbm, vel_hbm, lab_hbm, sidx_hbm, sval_hbm, small_hbm, large_hbm,
    out_d, out_v,
    send_buf, recv_buf, half_send, half_own, half_recv, back_send, back_recv,
    sound, mass, dens, vel, lab, sidx, sval, flat, mixed, large, turned_large,
    base_v, coef_v, base_d, coef_d, corr, row_of, col_of,
    send_sem, recv_sem, half_sem, half_got, back_sem, back_got, load_sem,
):
    gz = lax.axis_index("gz")
    gx = lax.axis_index("gx")
    core = lax.rem(gx, 2)
    me = gz * 2 + lax.div(gx, 2)
    partner = (gz, gx + 1 - 2 * core)

    loads = [
        pltpu.make_async_copy(away, here, load_sem.at[i])
        for i, (away, here) in enumerate(
            (
                (sound_hbm, sound),
                (lab_hbm, lab),
                (dens_hbm, dens),
                (small_hbm.at[0], flat),
                (mass_hbm, mass),
                (vel_hbm, vel),
                (sidx_hbm, sidx),
                (sval_hbm, sval),
                (small_hbm.at[1 + core], mixed),
                (large_hbm, large),
            )
        )
    ]
    for load in loads:
        load.start()

    own_low = lax.div(gx, 2)
    neighbour = (gz, gx + 2 - 4 * own_low)
    high, plane_x, plane_y = lax.div(gz, 16), lax.rem(lax.div(gz, 4), 4), lax.rem(gz, 4)
    ring = (2, 3, 1, 0)
    rows_y = [lax.rem(plane_y + o, 4) for o in ring]

    def each_peer(visit):
        def line(step, carry):
            t, u = lax.div(step, 4), lax.rem(step, 4)
            far_z = lax.rem(high + 2 + lax.div(t * (t + 1), 2), 4)
            far_x = lax.rem(plane_x + 2 + lax.div(u * (u + 1), 2), 4)
            for y in rows_y:
                at = far_z * 16 + far_x * 4 + y
                for low in range(2):
                    visit(at, low, (at, 2 * low + core))
            return carry

        lax.fori_loop(0, 15, line, 0)
        for y in rows_y[:3]:
            at = high * 16 + plane_x * 4 + y
            for low in range(2):
                visit(at, low, (at, 2 * low + core))
        visit(gz, 1 - own_low, neighbour)

    barrier = pltpu.get_barrier_semaphore()

    def greet(at, low, device):
        pl.semaphore_signal(barrier, inc=1, device_id=device, device_id_type=MESH)

    each_peer(greet)
    pl.semaphore_signal(barrier, inc=1, device_id=partner, device_id_type=MESH)

    def send(which):
        own = pl.ds(pl.multiple_of(me * 8, 8), 2)
        recv_buf[which, own, :] = send_buf[which, own, :]

        def one(at, low, device):
            pltpu.make_async_remote_copy(
                send_buf.at[which, pl.ds(pl.multiple_of(at * 16 + low * 8, 8), 2)],
                recv_buf.at[which, own],
                send_sem.at[which],
                recv_sem.at[which],
                device_id=device,
                device_id_type=MESH,
            ).start()

        each_peer(one)

    some = pl.ds(0, 2 * (CHIPS - 1))

    def arrived(which):
        pltpu.make_async_copy(
            send_buf.at[which, some], recv_buf.at[which, some], recv_sem.at[which]
        ).wait()

    def sent(which):
        pltpu.make_async_copy(
            send_buf.at[which, some], recv_buf.at[which, some], send_sem.at[which]
        ).wait()

    def put(which, value):
        for tile in range(2):
            send_buf[which, pl.ds(tile, CHIPS, stride=8), :] = value[:, tile * 128 : tile * 128 + 128]

    def turned(which):
        tiles = [recv_buf[which, pl.ds(tile, CHIPS, stride=8), :].T for tile in range(2)]
        return split(jnp.concatenate(tiles, axis=0))

    low = low_half((128, 128))
    low_32 = low_half((32, 128))

    def stacked(blocks):
        value = jnp.concatenate(blocks, axis=0)
        high = value.astype(BF16).astype(F32)
        return jnp.where(low_half(value.shape), value, value - high).astype(BF16)

    def long_product(tables, value):
        def dot(table):
            return jnp.dot(table, value, preferred_element_type=F32)

        return dot(tables[0]) + dot(tables[1])

    def combine(u, v, mask):
        return jnp.where(mask, u, v) + pltpu.roll(jnp.where(mask, v, u), 64, 1)

    core_sign = (1 - 2 * core).astype(F32)

    def get_slab(which, own):
        blocks = []
        for tile in range(2):
            near = [recv_buf[which, pl.ds(tile + 8 * at, 64, stride=16), :] for at in range(2)]
            b0, b1 = interleave(*[a[:32] + (core_sign if own else -core_sign) * a[32:] for a in near])
            q0, q2 = both(b0)
            q1, q3 = both(b1)
            blocks += [q0, q1, q2, q3]
        return stacked(blocks)

    def put_slab(which, folds):
        for tile in range(2):
            ends = []
            for value in folds:
                q = [value[(tile * 4 + i) * 32 : (tile * 4 + i) * 32 + 32] for i in range(4)]
                ends.append(interleave(combine(q[0], q[2], low_32), combine(q[1], q[3], low_32)))
            for at in range(2):
                first = tile + 8 * at
                send_buf[which, pl.ds(first, 32, stride=16), :] = ends[0][at] + ends[1][at]
                send_buf[which, pl.ds(first + 512, 32, stride=16), :] = core_sign * (
                    ends[0][at] - ends[1][at]
                )

    def along_z(table, value, own):
        half = core if own else 1 - core
        return long_product((table[half, 0], table[half, 1]), value)

    def give_half(which, make):
        value = make(False)
        half_send[which] = combine(value[:128], value[128:], low)
        copy = pltpu.make_async_remote_copy(
            half_send.at[which],
            half_recv.at[which],
            half_sem.at[which],
            half_got.at[which],
            device_id=partner,
            device_id_type=MESH,
        )
        copy.start()
        value = make(True)
        half_own[which] = combine(value[:128], value[128:], low)
        return copy

    def take_half(which, copy):
        copy.wait_recv()
        mine = half_own[which]
        other = half_recv[which]
        top = jnp.where(low, mine, pltpu.roll(other, 64, 1))
        bottom = jnp.where(low, pltpu.roll(mine, 64, 1), other)
        return split(jnp.concatenate([top, bottom], axis=0))

    def give_back(which, value):
        top, bottom = value[:128], value[128:]
        back_send[which] = jnp.where(low, pltpu.roll(top, 64, 1), bottom)
        copy = pltpu.make_async_remote_copy(
            back_send.at[which],
            back_recv.at[which],
            back_sem.at[which],
            back_got.at[which],
            device_id=partner,
            device_id_type=MESH,
        )
        copy.start()
        return copy, stacked(both(jnp.where(low, top, pltpu.roll(bottom, 64, 1))))

    def take_back(which, copy):
        copy.wait_recv()
        return stacked(both(back_recv[which]))

    for load in loads[:4]:
        load.wait()
    def r_flat():
        return flat[0], flat[1]

    def d_flat():
        return flat[2], flat[3]

    speed_ref = sound[0]
    for tissue in range(1, LABELS):
        speed_ref = jnp.maximum(speed_ref, sound[tissue])

    classes = lab[...].reshape(ROWS, NY)
    speed = jnp.full((ROWS, NY), sound[0])
    for tissue in range(1, LABELS):
        speed = jnp.where(classes == tissue, sound[tissue], speed)
    pressure = speed * speed * dens[...].reshape(ROWS, NY)
    put(P_S, product(r_flat, split(pressure), "nt"))
    pl.semaphore_wait(barrier, CHIPS)
    send(P_S)

    for load in loads[4:8]:
        load.wait()
    density_mass = jnp.full((ROWS, NY), mass[0])
    for tissue in range(1, LABELS):
        density_mass = jnp.where(classes == tissue, mass[tissue], density_mass)
    row = lax.broadcasted_iota(jnp.int32, (ROWS, NY), 0)
    col = lax.broadcasted_iota(jnp.int32, (ROWS, NY), 1)

    def damping(position, length):
        coordinate = position.astype(F32)
        depth = jnp.maximum(
            jnp.maximum(PML_W - coordinate, coordinate - (length - 1 - PML_W)), 0.0
        ) / PML_W
        square = depth * depth
        return jnp.exp(-ABSORB * speed_ref * (square * square) * DT * 0.5)

    damp = (
        damping(gz * Z_LOC + row // X_LOC, NZ),
        damping(gx * X_LOC + row % X_LOC, NX),
        damping(col, NY),
    )
    over_mass = DT / density_mass
    for a in range(3):
        base_v[a] = damp[a] * (damp[a] * vel[a].reshape(ROWS, NY))
        coef_v[a] = damp[a] * over_mass
    damp_all = damp[0] * damp[1] * damp[2]
    base_d[...] = damp_all * (damp_all * dens[...].reshape(ROWS, NY))
    coef_d[...] = damp_all * (DT * density_mass)

    line = lax.broadcasted_iota(jnp.int32, (256, NX), 0)
    index_x = lax.broadcasted_iota(jnp.int32, (256, NX), 1)

    def wave(index, length):
        folded = jnp.where(index <= length // 2, index, index - length // 2)
        return folded.astype(F32) * (2.0 * math.pi / length)

    folded = jnp.where(line <= 128 - core, line, line - 128)
    wz = (2 * folded + core).astype(F32) * (2.0 * math.pi / NZ)
    wx = wave(index_x, NX)
    wy = wave(jnp.full((256, NX), me, jnp.int32), NY)
    angle = speed_ref * jnp.sqrt(wz * wz + wx * wx + wy * wy) * (DT / 2.0)
    at_zero = angle == 0.0
    safe = jnp.where(at_zero, 1.0, angle)
    corr[...] = jnp.where(at_zero, 1.0, jnp.sin(safe) / safe)

    for load in loads[8:]:
        load.wait()
    for half in range(2):
        for table in range(4):
            turned_large[half, table] = large[half, table].T
    r_large, d_large = large.at[:, 0:2], large.at[:, 2:4]
    r_turned, d_turned = turned_large.at[:, 0:2], turned_large.at[:, 2:4]

    def r_mixed():
        return mixed[0], mixed[1]

    def d_mixed():
        return mixed[2], mixed[3]

    copies = []

    arrived(P_S)
    copy = give_half(P_C, lambda own: along_z(r_large, get_slab(P_S, own), own))
    copies.append(copy)
    spectrum = product(take_half(P_C, copy), r_mixed, "nt")
    spectrum = split(spectrum * corr[...])
    back_0, own_0 = give_back(V0_I, product(spectrum, r_mixed, "nn"))
    back_x, own_x = give_back(VX_I, product(spectrum, d_mixed, "nn"))
    copies += [back_0, back_x]
    part = along_z(r_turned, own_0, True)
    other_0 = take_back(V0_I, back_0)
    put_slab(U0_S, [part, along_z(r_turned, other_0, False)])
    send(U0_S)
    part = along_z(r_turned, own_x, True)
    put_slab(UX_S, [part, along_z(r_turned, take_back(VX_I, back_x), False)])
    send(UX_S)
    put_slab(UZ_S, [along_z(d_turned, own_0, True), along_z(d_turned, other_0, False)])
    send(UZ_S)

    where = sidx[...]
    plane = NX * NY
    z_off = where // plane - gz * Z_LOC
    remain = where % plane
    x_off = remain // NY - gx * X_LOC
    inside = (z_off >= 0) & (z_off < Z_LOC) & (x_off >= 0) & (x_off < X_LOC)
    row_of[...] = jnp.where(inside, z_off * X_LOC + x_off, -1)
    col_of[...] = remain % NY

    def add_some(step, carry):
        picks = []
        highs = []
        lows = []
        for part in range(2):
            at = pl.ds(step * 2 + part, 1)
            picks.append(jnp.where(row == row_of[at, :], 1.0, 0.0).astype(BF16))
            amount = jnp.where(row[:NY] == col_of[at, :], sval[at, :], 0.0)
            high, low = split(amount)
            highs.append(high)
            lows.append(low)
        pick = jnp.concatenate(picks, axis=1)
        contract = (((1,), (1,)), ((), ()))
        high = lax.dot_general(pick, jnp.concatenate(highs, axis=1), contract, preferred_element_type=F32)
        low = lax.dot_general(pick, jnp.concatenate(lows, axis=1), contract, preferred_element_type=F32)
        base_d[...] += high + low
        return carry

    lax.fori_loop(0, SRC // NY // 2, add_some, 0)

    for came, goes, a, back, sign in (
        (U0_S, VY_S, 2, d_flat, -1),
        (UX_S, VX_S, 1, r_flat, 1),
        (UZ_S, VZ_S, 0, r_flat, 1),
    ):
        arrived(came)
        slope = product(turned(came), back, "nn")
        fresh = base_v[a] - coef_v[a] * slope
        halves = split(fresh)
        if sign > 0:
            put(goes, product(r_flat, halves, "nt"))
        else:
            put(goes, -product(d_flat, halves, "nt"))
        send(goes)
        out_v[a] = fresh.reshape(Z_LOC, X_LOC, NY)

    arrived(VY_S)
    part_yz = [along_z(r_large, get_slab(VY_S, own), own) for own in (False, True)]
    arrived(VX_S)
    copy_x = give_half(X_C, lambda own: along_z(r_large, get_slab(VX_S, own), own))
    spectrum = product(take_half(X_C, copy_x), d_mixed, "nt")
    arrived(VZ_S)
    copy_yz = give_half(
        YZ_C, lambda own: part_yz[own] - along_z(d_large, get_slab(VZ_S, own), own)
    )
    spectrum = product(take_half(YZ_C, copy_yz), r_mixed, "nt") - spectrum
    back_e, own_e = give_back(E_I, product(split(spectrum * corr[...]), r_mixed, "nn"))
    copies += [copy_x, copy_yz, back_e]
    part = along_z(r_turned, own_e, True)
    put_slab(E_S, [part, along_z(r_turned, take_back(E_I, back_e), False)])
    send(E_S)

    arrived(E_S)
    spread = product(turned(E_S), r_flat, "nn")
    out_d[...] = (base_d[...] - coef_d[...] * spread).reshape(Z_LOC, X_LOC, NY)
    for which in range(8):
        sent(which)
    for copy in copies:
        copy.wait_send()


def shards(density, velocity, labels, sound_table, mass_table, source_index, source_values):
    small, large = tables()
    vmem = pl.BlockSpec(memory_space=pltpu.VMEM)
    hbm = pl.BlockSpec(memory_space=pl.ANY)
    field = (Z_LOC, X_LOC, NY)
    return pl.pallas_call(
        kernel,
        out_shape=(
            pltpu.VMEM(field, F32),
            pltpu.VMEM((3,) + field, F32),
        ),
        in_specs=[hbm] * 9,
        out_specs=(vmem, vmem),
        scratch_shapes=[
            pltpu.VMEM((8, WIDE, 128), F32),
            pltpu.VMEM((8, WIDE, 128), F32),
            pltpu.VMEM((3, 128, 128), F32),
            pltpu.VMEM((3, 128, 128), F32),
            pltpu.VMEM((3, 128, 128), F32),
            pltpu.VMEM((3, 128, 128), F32),
            pltpu.VMEM((3, 128, 128), F32),
            pltpu.SMEM((LABELS,), F32),
            pltpu.SMEM((LABELS,), F32),
            pltpu.VMEM(field, F32),
            pltpu.VMEM((3,) + field, F32),
            pltpu.VMEM(field, jnp.int32),
            pltpu.VMEM((SRC // NY, NY), jnp.int32),
            pltpu.VMEM((SRC // NY, NY), F32),
            pltpu.VMEM((4, NX, NX), BF16),
            pltpu.VMEM((4, NX, NX), BF16),
            pltpu.VMEM((2, 4, NZ // 2, NZ // 2), BF16),
            pltpu.VMEM((2, 4, NZ // 2, NZ // 2), BF16),
            pltpu.VMEM((3, ROWS, NY), F32),
            pltpu.VMEM((3, ROWS, NY), F32),
            pltpu.VMEM((ROWS, NY), F32),
            pltpu.VMEM((ROWS, NY), F32),
            pltpu.VMEM((256, NX), F32),
            pltpu.VMEM((SRC // NY, NY), jnp.int32),
            pltpu.VMEM((SRC // NY, NY), jnp.int32),
            pltpu.SemaphoreType.DMA((8,)),
            pltpu.SemaphoreType.DMA((8,)),
            pltpu.SemaphoreType.DMA((3,)),
            pltpu.SemaphoreType.DMA((3,)),
            pltpu.SemaphoreType.DMA((3,)),
            pltpu.SemaphoreType.DMA((3,)),
            pltpu.SemaphoreType.DMA((10,)),
        ],
        compiler_params=pltpu.CompilerParams(collective_id=0, has_side_effects=True),
    )(
        sound_table,
        mass_table,
        density,
        velocity,
        labels,
        source_index.reshape(SRC // NY, NY),
        source_values[0].reshape(SRC // NY, NY),
        jnp.asarray(small),
        jnp.asarray(large),
    )


def solution(mesh):
    in_specs = (
        P("gz", "gx", None),
        P(None, "gz", "gx", None),
        P("gz", "gx", None),
        P(),
        P(),
        P(),
        P(),
    )
    out_specs = (P("gz", "gx", None), P(None, "gz", "gx", None))
    return jax.shard_map(shards, mesh=mesh, in_specs=in_specs, out_specs=out_specs, check_vma=False)
```

```python
import math

import jax
import jax.numpy as jnp
import numpy as np
from jax import lax
from jax.experimental import pallas as pl
from jax.experimental.pallas import tpu as pltpu
from jax.sharding import PartitionSpec as P

NZ = 512
NX = 128
NY = 128
LABELS = 8
PML_W = 20
SRC = 4096
DT = 0.3
ABSORB = 2.0
CHIPS = 128
WIDE = CHIPS * 8
Z_LOC = 8
X_LOC = 32
ROWS = Z_LOC * X_LOC
MESH = pl.DeviceIdType.MESH
F32 = jnp.float32
BF16 = jnp.bfloat16

P_S, U0_S, UX_S, UZ_S, VY_S, VX_S, VZ_S, E_S = range(8)
P_C, X_C, YZ_C = range(3)
V0_I, VX_I, E_I = range(3)


def basis(n):
    j = np.arange(n)
    f = np.concatenate([np.arange(n // 2 + 1), np.arange(1, n // 2)])
    is_sin = (np.arange(n) > n // 2)[:, None]
    scale = np.where((f == 0) | (f == n // 2), math.sqrt(1.0 / n), math.sqrt(2.0 / n))[:, None]
    k = (2.0 * math.pi / n * f)[:, None]
    phase = 2.0 * math.pi / n * ((f[:, None] * j[None, :]) % n)
    half = 2.0 * math.pi / (2 * n) * ((f[:, None] * (2 * j[None, :] + 1)) % (2 * n))
    forward = np.where(is_sin, np.sin(phase), np.cos(phase)) * scale
    slope = np.where(is_sin, k * np.cos(half), -k * np.sin(half)) * scale
    return forward, slope


def parts(table):
    table = table.astype(np.float32)
    high = table.astype(jnp.bfloat16)
    low = (table - high.astype(np.float32)).astype(jnp.bfloat16)
    return [high, low]


def tables():
    r, d = basis(NX)
    lane = np.arange(NX)
    x_of = [((lane % 64) // 32 * 2 + (lane // 64 + core) % 2) * X_LOC + lane % 32 for core in range(2)]
    small = np.stack([np.stack(parts(r[:, x]) + parts(d[:, x])) for x in [lane] + x_of])
    r, d = basis(NZ)
    frequency = np.concatenate([np.arange(NZ // 2 + 1), np.arange(1, NZ // 2)])
    row = np.arange(NZ // 2)
    z = (row % 32) * Z_LOC + row // 32
    large = np.stack(
        [
            np.stack(parts(r[frequency % 2 == odd][:, z]) + parts(d[frequency % 2 == odd][:, z]))
            for odd in range(2)
        ]
    )
    return small, large


def split(x):
    high = x.astype(BF16)
    return high, (x - high.astype(F32)).astype(BF16)


def product(a, b, dims):
    contract = (((1,), (0 if dims == "nn" else 1,)), ((), ()))
    a, b = (x() if callable(x) else x for x in (a, b))

    def dot(u, v):
        return lax.dot_general(u, v, contract, preferred_element_type=F32)

    return dot(a[0], b[0]) + dot(a[1], b[0]) + dot(a[0], b[1])


def interleave(u, v):
    even = lax.broadcasted_iota(jnp.int32, u.shape, 1) % 64 < 32
    return jnp.where(even, u, pltpu.roll(v, 32, 1)), jnp.where(even, pltpu.roll(u, 96, 1), v)


def low_half(shape):
    return lax.broadcasted_iota(jnp.int32, shape, 1) < 64


def both(u):
    low = low_half(u.shape)
    other = pltpu.roll(u, 64, 1)
    return jnp.where(low, u, other), jnp.where(low, other, u)


def kernel(
    sound_hbm, mass_hbm, dens_hbm, vel_hbm, lab_hbm, sidx_hbm, sval_hbm, small_hbm, large_hbm,
    out_d, out_v,
    send_buf, recv_buf, half_send, half_own, half_recv, back_send, back_recv,
    sound, mass, dens, vel, lab, sidx, sval, flat, mixed, large, turned_large,
    base_v, coef_v, base_d, coef_d, corr, row_of, col_of,
    send_sem, recv_sem, half_sem, half_got, back_sem, back_got, load_sem,
):
    gz = lax.axis_index("gz")
    gx = lax.axis_index("gx")
    core = lax.rem(gx, 2)
    me = gz * 2 + lax.div(gx, 2)
    partner = (gz, gx + 1 - 2 * core)

    loads = [
        pltpu.make_async_copy(away, here, load_sem.at[i])
        for i, (away, here) in enumerate(
            (
                (sound_hbm, sound),
                (lab_hbm, lab),
                (dens_hbm, dens),
                (small_hbm.at[0], flat),
                (mass_hbm, mass),
                (vel_hbm, vel),
                (sidx_hbm, sidx),
                (sval_hbm, sval),
                (small_hbm.at[1 + core], mixed),
                (large_hbm, large),
            )
        )
    ]
    for load in loads:
        load.start()

    own_low = lax.div(gx, 2)
    neighbour = (gz, gx + 2 - 4 * own_low)
    high, plane_x, plane_y = lax.div(gz, 16), lax.rem(lax.div(gz, 4), 4), lax.rem(gz, 4)
    ring = (2, 3, 1, 0)
    rows_y = [lax.rem(plane_y + o, 4) for o in ring]

    def each_peer(visit):
        def lines(first, last, far):
            rows_z = [lax.rem(high + z, 4) for z in far]

            def line(step, carry):
                far_x = lax.rem(plane_x + 2 + lax.div(step * (step + 1), 2), 4)
                for y in rows_y:
                    for z in rows_z:
                        at = z * 16 + far_x * 4 + y
                        for low in range(2):
                            visit(at, low, (at, 2 * low + core))
                return carry

            lax.fori_loop(first, last, line, 0)

        lines(0, 4, (2, 3, 1))
        lines(0, 3, (0,))
        for y in rows_y[:3]:
            at = high * 16 + plane_x * 4 + y
            for low in range(2):
                visit(at, low, (at, 2 * low + core))
        visit(gz, 1 - own_low, neighbour)

    barrier = pltpu.get_barrier_semaphore()

    def greet(at, low, device):
        pl.semaphore_signal(barrier, inc=1, device_id=device, device_id_type=MESH)

    each_peer(greet)
    pl.semaphore_signal(barrier, inc=1, device_id=partner, device_id_type=MESH)

    def send(which):
        own = pl.ds(pl.multiple_of(me * 8, 8), 2)
        recv_buf[which, own, :] = send_buf[which, own, :]

        def one(at, low, device):
            pltpu.make_async_remote_copy(
                send_buf.at[which, pl.ds(pl.multiple_of(at * 16 + low * 8, 8), 2)],
                recv_buf.at[which, own],
                send_sem.at[which],
                recv_sem.at[which],
                device_id=device,
                device_id_type=MESH,
            ).start()

        each_peer(one)

    some = pl.ds(0, 2 * (CHIPS - 1))

    def arrived(which):
        pltpu.make_async_copy(
            send_buf.at[which, some], recv_buf.at[which, some], recv_sem.at[which]
        ).wait()

    def sent(which):
        pltpu.make_async_copy(
            send_buf.at[which, some], recv_buf.at[which, some], send_sem.at[which]
        ).wait()

    def put(which, value):
        for tile in range(2):
            send_buf[which, pl.ds(tile, CHIPS, stride=8), :] = value[:, tile * 128 : tile * 128 + 128]

    def turned(which):
        tiles = [recv_buf[which, pl.ds(tile, CHIPS, stride=8), :].T for tile in range(2)]
        return split(jnp.concatenate(tiles, axis=0))

    low = low_half((128, 128))
    low_32 = low_half((32, 128))

    def stacked(blocks):
        value = jnp.concatenate(blocks, axis=0)
        high = value.astype(BF16).astype(F32)
        return jnp.where(low_half(value.shape), value, value - high).astype(BF16)

    def long_product(tables, value):
        def dot(table):
            return jnp.dot(table, value, preferred_element_type=F32)

        return dot(tables[0]) + dot(tables[1])

    def combine(u, v, mask):
        return jnp.where(mask, u, v) + pltpu.roll(jnp.where(mask, v, u), 64, 1)

    core_sign = (1 - 2 * core).astype(F32)

    def get_slab(which, own):
        blocks = []
        for tile in range(2):
            near = [recv_buf[which, pl.ds(tile + 8 * at, 64, stride=16), :] for at in range(2)]
            b0, b1 = interleave(*[a[:32] + (core_sign if own else -core_sign) * a[32:] for a in near])
            q0, q2 = both(b0)
            q1, q3 = both(b1)
            blocks += [q0, q1, q2, q3]
        return stacked(blocks)

    def put_slab(which, folds):
        for tile in range(2):
            ends = []
            for value in folds:
                q = [value[(tile * 4 + i) * 32 : (tile * 4 + i) * 32 + 32] for i in range(4)]
                ends.append(interleave(combine(q[0], q[2], low_32), combine(q[1], q[3], low_32)))
            for at in range(2):
                first = tile + 8 * at
                send_buf[which, pl.ds(first, 32, stride=16), :] = ends[0][at] + ends[1][at]
                send_buf[which, pl.ds(first + 512, 32, stride=16), :] = core_sign * (
                    ends[0][at] - ends[1][at]
                )

    def along_z(table, value, own):
        half = core if own else 1 - core
        return long_product((table[half, 0], table[half, 1]), value)

    def give_half(which, make):
        value = make(False)
        half_send[which] = combine(value[:128], value[128:], low)
        copy = pltpu.make_async_remote_copy(
            half_send.at[which],
            half_recv.at[which],
            half_sem.at[which],
            half_got.at[which],
            device_id=partner,
            device_id_type=MESH,
        )
        copy.start()
        value = make(True)
        half_own[which] = combine(value[:128], value[128:], low)
        return copy

    def take_half(which, copy):
        copy.wait_recv()
        mine = half_own[which]
        other = half_recv[which]
        top = jnp.where(low, mine, pltpu.roll(other, 64, 1))
        bottom = jnp.where(low, pltpu.roll(mine, 64, 1), other)
        return split(jnp.concatenate([top, bottom], axis=0))

    def give_back(which, value):
        top, bottom = value[:128], value[128:]
        back_send[which] = jnp.where(low, pltpu.roll(top, 64, 1), bottom)
        copy = pltpu.make_async_remote_copy(
            back_send.at[which],
            back_recv.at[which],
            back_sem.at[which],
            back_got.at[which],
            device_id=partner,
            device_id_type=MESH,
        )
        copy.start()
        return copy, stacked(both(jnp.where(low, top, pltpu.roll(bottom, 64, 1))))

    def take_back(which, copy):
        copy.wait_recv()
        return stacked(both(back_recv[which]))

    for load in loads[:4]:
        load.wait()
    def r_flat():
        return flat[0], flat[1]

    def d_flat():
        return flat[2], flat[3]

    speed_ref = sound[0]
    for tissue in range(1, LABELS):
        speed_ref = jnp.maximum(speed_ref, sound[tissue])

    classes = lab[...].reshape(ROWS, NY)
    speed = jnp.full((ROWS, NY), sound[0])
    for tissue in range(1, LABELS):
        speed = jnp.where(classes == tissue, sound[tissue], speed)
    pressure = speed * speed * dens[...].reshape(ROWS, NY)
    put(P_S, product(r_flat, split(pressure), "nt"))
    pl.semaphore_wait(barrier, CHIPS)
    send(P_S)

    for load in loads[4:8]:
        load.wait()
    density_mass = jnp.full((ROWS, NY), mass[0])
    for tissue in range(1, LABELS):
        density_mass = jnp.where(classes == tissue, mass[tissue], density_mass)
    row = lax.broadcasted_iota(jnp.int32, (ROWS, NY), 0)
    col = lax.broadcasted_iota(jnp.int32, (ROWS, NY), 1)

    def damping(position, length):
        coordinate = position.astype(F32)
        depth = jnp.maximum(
            jnp.maximum(PML_W - coordinate, coordinate - (length - 1 - PML_W)), 0.0
        ) / PML_W
        square = depth * depth
        return jnp.exp(-ABSORB * speed_ref * (square * square) * DT * 0.5)

    damp = (
        damping(gz * Z_LOC + row // X_LOC, NZ),
        damping(gx * X_LOC + row % X_LOC, NX),
        damping(col, NY),
    )
    over_mass = DT / density_mass
    for a in range(3):
        base_v[a] = damp[a] * (damp[a] * vel[a].reshape(ROWS, NY))
        coef_v[a] = damp[a] * over_mass
    damp_all = damp[0] * damp[1] * damp[2]
    base_d[...] = damp_all * (damp_all * dens[...].reshape(ROWS, NY))
    coef_d[...] = damp_all * (DT * density_mass)

    line = lax.broadcasted_iota(jnp.int32, (256, NX), 0)
    index_x = lax.broadcasted_iota(jnp.int32, (256, NX), 1)

    def wave(index, length):
        folded = jnp.where(index <= length // 2, index, index - length // 2)
        return folded.astype(F32) * (2.0 * math.pi / length)

    folded = jnp.where(line <= 128 - core, line, line - 128)
    wz = (2 * folded + core).astype(F32) * (2.0 * math.pi / NZ)
    wx = wave(index_x, NX)
    wy = wave(jnp.full((256, NX), me, jnp.int32), NY)
    angle = speed_ref * jnp.sqrt(wz * wz + wx * wx + wy * wy) * (DT / 2.0)
    at_zero = angle == 0.0
    safe = jnp.where(at_zero, 1.0, angle)
    corr[...] = jnp.where(at_zero, 1.0, jnp.sin(safe) / safe)

    for load in loads[8:]:
        load.wait()
    for half in range(2):
        for table in range(4):
            turned_large[half, table] = large[half, table].T
    r_large, d_large = large.at[:, 0:2], large.at[:, 2:4]
    r_turned, d_turned = turned_large.at[:, 0:2], turned_large.at[:, 2:4]

    def r_mixed():
        return mixed[0], mixed[1]

    def d_mixed():
        return mixed[2], mixed[3]

    copies = []

    arrived(P_S)
    copy = give_half(P_C, lambda own: along_z(r_large, get_slab(P_S, own), own))
    copies.append(copy)
    spectrum = product(take_half(P_C, copy), r_mixed, "nt")
    spectrum = split(spectrum * corr[...])
    back_0, own_0 = give_back(V0_I, product(spectrum, r_mixed, "nn"))
    back_x, own_x = give_back(VX_I, product(spectrum, d_mixed, "nn"))
    copies += [back_0, back_x]
    part = along_z(r_turned, own_0, True)
    other_0 = take_back(V0_I, back_0)
    put_slab(U0_S, [part, along_z(r_turned, other_0, False)])
    send(U0_S)
    part = along_z(r_turned, own_x, True)
    put_slab(UX_S, [part, along_z(r_turned, take_back(VX_I, back_x), False)])
    send(UX_S)
    put_slab(UZ_S, [along_z(d_turned, own_0, True), along_z(d_turned, other_0, False)])
    send(UZ_S)

    where = sidx[...]
    plane = NX * NY
    z_off = where // plane - gz * Z_LOC
    remain = where % plane
    x_off = remain // NY - gx * X_LOC
    inside = (z_off >= 0) & (z_off < Z_LOC) & (x_off >= 0) & (x_off < X_LOC)
    row_of[...] = jnp.where(inside, z_off * X_LOC + x_off, -1)
    col_of[...] = remain % NY

    def add_some(step, carry):
        picks = []
        highs = []
        lows = []
        for part in range(2):
            at = pl.ds(step * 2 + part, 1)
            picks.append(jnp.where(row == row_of[at, :], 1.0, 0.0).astype(BF16))
            amount = jnp.where(row[:NY] == col_of[at, :], sval[at, :], 0.0)
            high, low = split(amount)
            highs.append(high)
            lows.append(low)
        pick = jnp.concatenate(picks, axis=1)
        contract = (((1,), (1,)), ((), ()))
        high = lax.dot_general(pick, jnp.concatenate(highs, axis=1), contract, preferred_element_type=F32)
        low = lax.dot_general(pick, jnp.concatenate(lows, axis=1), contract, preferred_element_type=F32)
        base_d[...] += high + low
        return carry

    lax.fori_loop(0, SRC // NY // 2, add_some, 0)

    for came, goes, a, back, sign in (
        (U0_S, VY_S, 2, d_flat, -1),
        (UX_S, VX_S, 1, r_flat, 1),
        (UZ_S, VZ_S, 0, r_flat, 1),
    ):
        arrived(came)
        slope = product(turned(came), back, "nn")
        fresh = base_v[a] - coef_v[a] * slope
        halves = split(fresh)
        if sign > 0:
            put(goes, product(r_flat, halves, "nt"))
        else:
            put(goes, -product(d_flat, halves, "nt"))
        send(goes)
        out_v[a] = fresh.reshape(Z_LOC, X_LOC, NY)

    arrived(VY_S)
    part_yz = [along_z(r_large, get_slab(VY_S, own), own) for own in (False, True)]
    arrived(VX_S)
    copy_x = give_half(X_C, lambda own: along_z(r_large, get_slab(VX_S, own), own))
    spectrum = product(take_half(X_C, copy_x), d_mixed, "nt")
    arrived(VZ_S)
    copy_yz = give_half(
        YZ_C, lambda own: part_yz[own] - along_z(d_large, get_slab(VZ_S, own), own)
    )
    spectrum = product(take_half(YZ_C, copy_yz), r_mixed, "nt") - spectrum
    back_e, own_e = give_back(E_I, product(split(spectrum * corr[...]), r_mixed, "nn"))
    copies += [copy_x, copy_yz, back_e]
    part = along_z(r_turned, own_e, True)
    put_slab(E_S, [part, along_z(r_turned, take_back(E_I, back_e), False)])
    send(E_S)

    arrived(E_S)
    spread = product(turned(E_S), r_flat, "nn")
    out_d[...] = (base_d[...] - coef_d[...] * spread).reshape(Z_LOC, X_LOC, NY)
    for which in range(8):
        sent(which)
    for copy in copies:
        copy.wait_send()


def write_out(new_d, new_v, out_d, out_v, out_sem):
    copies = [
        pltpu.make_async_copy(here, away, out_sem.at[i])
        for i, (here, away) in enumerate(((new_v, out_v), (new_d, out_d)))
    ]
    for copy in copies:
        copy.start()
    for copy in copies:
        copy.wait()


def shards(density, velocity, labels, sound_table, mass_table, source_index, source_values):
    small, large = tables()
    vmem = pl.BlockSpec(memory_space=pltpu.VMEM)
    hbm = pl.BlockSpec(memory_space=pl.ANY)
    field = (Z_LOC, X_LOC, NY)
    results = pl.pallas_call(
        kernel,
        out_shape=(
            pltpu.VMEM(field, F32),
            pltpu.VMEM((3,) + field, F32),
        ),
        in_specs=[hbm] * 9,
        out_specs=(vmem, vmem),
        scratch_shapes=[
            pltpu.VMEM((8, WIDE, 128), F32),
            pltpu.VMEM((8, WIDE, 128), F32),
            pltpu.VMEM((3, 128, 128), F32),
            pltpu.VMEM((3, 128, 128), F32),
            pltpu.VMEM((3, 128, 128), F32),
            pltpu.VMEM((3, 128, 128), F32),
            pltpu.VMEM((3, 128, 128), F32),
            pltpu.SMEM((LABELS,), F32),
            pltpu.SMEM((LABELS,), F32),
            pltpu.VMEM(field, F32),
            pltpu.VMEM((3,) + field, F32),
            pltpu.VMEM(field, jnp.int32),
            pltpu.VMEM((SRC // NY, NY), jnp.int32),
            pltpu.VMEM((SRC // NY, NY), F32),
            pltpu.VMEM((4, NX, NX), BF16),
            pltpu.VMEM((4, NX, NX), BF16),
            pltpu.VMEM((2, 4, NZ // 2, NZ // 2), BF16),
            pltpu.VMEM((2, 4, NZ // 2, NZ // 2), BF16),
            pltpu.VMEM((3, ROWS, NY), F32),
            pltpu.VMEM((3, ROWS, NY), F32),
            pltpu.VMEM((ROWS, NY), F32),
            pltpu.VMEM((ROWS, NY), F32),
            pltpu.VMEM((256, NX), F32),
            pltpu.VMEM((SRC // NY, NY), jnp.int32),
            pltpu.VMEM((SRC // NY, NY), jnp.int32),
            pltpu.SemaphoreType.DMA((8,)),
            pltpu.SemaphoreType.DMA((8,)),
            pltpu.SemaphoreType.DMA((3,)),
            pltpu.SemaphoreType.DMA((3,)),
            pltpu.SemaphoreType.DMA((3,)),
            pltpu.SemaphoreType.DMA((3,)),
            pltpu.SemaphoreType.DMA((10,)),
        ],
        compiler_params=pltpu.CompilerParams(collective_id=0, has_side_effects=True),
    )(
        sound_table,
        mass_table,
        density,
        velocity,
        labels,
        source_index.reshape(SRC // NY, NY),
        source_values[0].reshape(SRC // NY, NY),
        jnp.asarray(small),
        jnp.asarray(large),
    )

    return pl.pallas_call(
        write_out,
        out_shape=(
            jax.ShapeDtypeStruct(field, F32),
            jax.ShapeDtypeStruct((3,) + field, F32),
        ),
        in_specs=[vmem, vmem],
        out_specs=(hbm, hbm),
        scratch_shapes=[pltpu.SemaphoreType.DMA((2,))],
    )(*[pltpu.with_memory_space_constraint(result, pltpu.VMEM) for result in results])


def solution(mesh):
    in_specs = (
        P("gz", "gx", None),
        P(None, "gz", "gx", None),
        P("gz", "gx", None),
        P(),
        P(),
        P(),
        P(),
    )
    out_specs = (P("gz", "gx", None), P(None, "gz", "gx", None))
    return jax.shard_map(shards, mesh=mesh, in_specs=in_specs, out_specs=out_specs, check_vma=False)
```

```python
import math

import jax
import jax.numpy as jnp
import numpy as np
from jax import lax
from jax.experimental import pallas as pl
from jax.experimental.pallas import tpu as pltpu
from jax.sharding import PartitionSpec as P

NZ = 512
NX = 128
NY = 128
LABELS = 8
PML_W = 20
SRC = 4096
DT = 0.3
ABSORB = 2.0
CHIPS = 128
WIDE = CHIPS * 8
Z_LOC = 8
X_LOC = 32
ROWS = Z_LOC * X_LOC
MESH = pl.DeviceIdType.MESH
F32 = jnp.float32
BF16 = jnp.bfloat16

P_S, U0_S, UX_S, UZ_S, VY_S, VX_S, VZ_S, E_S = range(8)
P_C, X_C, YZ_C = range(3)
V0_I, VX_I, E_I = range(3)


def basis(n):
    j = np.arange(n)
    f = np.concatenate([np.arange(n // 2 + 1), np.arange(1, n // 2)])
    is_sin = (np.arange(n) > n // 2)[:, None]
    scale = np.where((f == 0) | (f == n // 2), math.sqrt(1.0 / n), math.sqrt(2.0 / n))[:, None]
    k = (2.0 * math.pi / n * f)[:, None]
    phase = 2.0 * math.pi / n * ((f[:, None] * j[None, :]) % n)
    half = 2.0 * math.pi / (2 * n) * ((f[:, None] * (2 * j[None, :] + 1)) % (2 * n))
    forward = np.where(is_sin, np.sin(phase), np.cos(phase)) * scale
    slope = np.where(is_sin, k * np.cos(half), -k * np.sin(half)) * scale
    return forward, slope


def parts(table):
    table = table.astype(np.float32)
    high = table.astype(jnp.bfloat16)
    low = (table - high.astype(np.float32)).astype(jnp.bfloat16)
    return [high, low]


def tables():
    r, d = basis(NX)
    lane = np.arange(NX)
    x_of = [((lane % 64) // 32 * 2 + (lane // 64 + core) % 2) * X_LOC + lane % 32 for core in range(2)]
    small = np.stack([np.stack(parts(r[:, x]) + parts(d[:, x])) for x in [lane] + x_of])
    r, d = basis(NZ)
    frequency = np.concatenate([np.arange(NZ // 2 + 1), np.arange(1, NZ // 2)])
    row = np.arange(NZ // 2)
    z = (row % 32) * Z_LOC + row // 32
    large = np.stack(
        [
            np.stack(parts(r[frequency % 2 == odd][:, z]) + parts(d[frequency % 2 == odd][:, z]))
            for odd in range(2)
        ]
    )
    return small, large


def split(x):
    high = x.astype(BF16)
    return high, (x - high.astype(F32)).astype(BF16)


def product(a, b, dims):
    contract = (((1,), (0 if dims == "nn" else 1,)), ((), ()))
    a, b = (x() if callable(x) else x for x in (a, b))

    def dot(u, v):
        return lax.dot_general(u, v, contract, preferred_element_type=F32)

    return dot(a[0], b[0]) + dot(a[1], b[0]) + dot(a[0], b[1])


def interleave(u, v):
    even = lax.broadcasted_iota(jnp.int32, u.shape, 1) % 64 < 32
    return jnp.where(even, u, pltpu.roll(v, 32, 1)), jnp.where(even, pltpu.roll(u, 96, 1), v)


def low_half(shape):
    return lax.broadcasted_iota(jnp.int32, shape, 1) < 64


def both(u):
    low = low_half(u.shape)
    other = pltpu.roll(u, 64, 1)
    return jnp.where(low, u, other), jnp.where(low, other, u)


def kernel(
    sound_hbm, mass_hbm, dens_hbm, vel_hbm, lab_hbm, sidx_hbm, sval_hbm, small_hbm, large_hbm,
    out_d, out_v,
    send_buf, recv_buf, half_send, half_own, half_recv, back_send, back_recv,
    sound, mass, dens, vel, lab, sidx, sval, flat, mixed, large, turned_large,
    base_v, coef_v, base_d, coef_d, corr, row_of, col_of,
    send_sem, recv_sem, half_sem, half_got, back_sem, back_got, load_sem,
):
    gz = lax.axis_index("gz")
    gx = lax.axis_index("gx")
    core = lax.rem(gx, 2)
    me = gz * 2 + lax.div(gx, 2)
    partner = (gz, gx + 1 - 2 * core)

    loads = [
        pltpu.make_async_copy(away, here, load_sem.at[i])
        for i, (away, here) in enumerate(
            (
                (sound_hbm, sound),
                (lab_hbm, lab),
                (dens_hbm, dens),
                (small_hbm.at[0], flat),
                (mass_hbm, mass),
                (vel_hbm, vel),
                (sidx_hbm, sidx),
                (sval_hbm, sval),
                (small_hbm.at[1 + core], mixed),
                (large_hbm, large),
            )
        )
    ]
    for load in loads:
        load.start()

    own_low = lax.div(gx, 2)
    neighbour = (gz, gx + 2 - 4 * own_low)
    high, plane_x, plane_y = lax.div(gz, 16), lax.rem(lax.div(gz, 4), 4), lax.rem(gz, 4)
    ring = (2, 3, 1, 0)
    rows_y = [lax.rem(plane_y + o, 4) for o in ring]

    def each_peer(visit):
        def lines(first, last, far):
            rows_z = [lax.rem(high + z, 4) for z in far]

            def line(step, carry):
                far_x = lax.rem(plane_x + 2 + lax.div(step * (step + 1), 2), 4)
                for y in rows_y:
                    for z in rows_z:
                        at = z * 16 + far_x * 4 + y
                        for low in range(2):
                            visit(at, low, (at, 2 * low + core))
                return carry

            lax.fori_loop(first, last, line, 0)

        lines(0, 4, (2, 3, 1))
        lines(0, 3, (0,))
        for y in rows_y[:3]:
            at = high * 16 + plane_x * 4 + y
            for low in range(2):
                visit(at, low, (at, 2 * low + core))
        visit(gz, 1 - own_low, neighbour)

    barrier = pltpu.get_barrier_semaphore()

    def greet(at, low, device):
        pl.semaphore_signal(barrier, inc=1, device_id=device, device_id_type=MESH)

    each_peer(greet)
    pl.semaphore_signal(barrier, inc=1, device_id=partner, device_id_type=MESH)

    def send(which):
        own = pl.ds(pl.multiple_of(me * 8, 8), 2)
        recv_buf[which, own, :] = send_buf[which, own, :]

        def one(at, low, device):
            pltpu.make_async_remote_copy(
                send_buf.at[which, pl.ds(pl.multiple_of(at * 16 + low * 8, 8), 2)],
                recv_buf.at[which, own],
                send_sem.at[which],
                recv_sem.at[which],
                device_id=device,
                device_id_type=MESH,
            ).start()

        each_peer(one)

    some = pl.ds(0, 2 * (CHIPS - 1))

    def arrived(which):
        pltpu.make_async_copy(
            send_buf.at[which, some], recv_buf.at[which, some], recv_sem.at[which]
        ).wait()

    def sent(which):
        pltpu.make_async_copy(
            send_buf.at[which, some], recv_buf.at[which, some], send_sem.at[which]
        ).wait()

    def put(which, value):
        for tile in range(2):
            send_buf[which, pl.ds(tile, CHIPS, stride=8), :] = value[:, tile * 128 : tile * 128 + 128]

    def turned(which):
        tiles = [recv_buf[which, pl.ds(tile, CHIPS, stride=8), :].T for tile in range(2)]
        return split(jnp.concatenate(tiles, axis=0))

    low = low_half((128, 128))
    low_32 = low_half((32, 128))

    def stacked(blocks):
        value = jnp.concatenate(blocks, axis=0)
        high = value.astype(BF16).astype(F32)
        return jnp.where(low_half(value.shape), value, value - high).astype(BF16)

    def long_product(tables, value):
        def dot(table):
            return jnp.dot(table, value, preferred_element_type=F32)

        return dot(tables[0]) + dot(tables[1])

    def combine(u, v, mask):
        return jnp.where(mask, u, v) + pltpu.roll(jnp.where(mask, v, u), 64, 1)

    core_sign = (1 - 2 * core).astype(F32)

    def get_slab(which, own):
        blocks = []
        for tile in range(2):
            near = [recv_buf[which, pl.ds(tile + 8 * at, 64, stride=16), :] for at in range(2)]
            b0, b1 = interleave(*[a[:32] + (core_sign if own else -core_sign) * a[32:] for a in near])
            q0, q2 = both(b0)
            q1, q3 = both(b1)
            blocks += [q0, q1, q2, q3]
        return stacked(blocks)

    def put_slab(which, folds):
        for tile in range(2):
            ends = []
            for value in folds:
                q = [value[(tile * 4 + i) * 32 : (tile * 4 + i) * 32 + 32] for i in range(4)]
                ends.append(interleave(combine(q[0], q[2], low_32), combine(q[1], q[3], low_32)))
            for at in range(2):
                first = tile + 8 * at
                send_buf[which, pl.ds(first, 32, stride=16), :] = ends[0][at] + ends[1][at]
                send_buf[which, pl.ds(first + 512, 32, stride=16), :] = core_sign * (
                    ends[0][at] - ends[1][at]
                )

    def along_z(table, value, own):
        half = core if own else 1 - core
        return long_product((table[half, 0], table[half, 1]), value)

    def give_half(which, make):
        value = make(False)
        half_send[which] = combine(value[:128], value[128:], low)
        copy = pltpu.make_async_remote_copy(
            half_send.at[which],
            half_recv.at[which],
            half_sem.at[which],
            half_got.at[which],
            device_id=partner,
            device_id_type=MESH,
        )
        copy.start()
        value = make(True)
        half_own[which] = combine(value[:128], value[128:], low)
        return copy

    def take_half(which, copy):
        copy.wait_recv()
        mine = half_own[which]
        other = half_recv[which]
        top = jnp.where(low, mine, pltpu.roll(other, 64, 1))
        bottom = jnp.where(low, pltpu.roll(mine, 64, 1), other)
        return split(jnp.concatenate([top, bottom], axis=0))

    def give_back(which, value):
        top, bottom = value[:128], value[128:]
        back_send[which] = jnp.where(low, pltpu.roll(top, 64, 1), bottom)
        copy = pltpu.make_async_remote_copy(
            back_send.at[which],
            back_recv.at[which],
            back_sem.at[which],
            back_got.at[which],
            device_id=partner,
            device_id_type=MESH,
        )
        copy.start()
        return copy, stacked(both(jnp.where(low, top, pltpu.roll(bottom, 64, 1))))

    def take_back(which, copy):
        copy.wait_recv()
        return stacked(both(back_recv[which]))

    for load in loads[:4]:
        load.wait()
    def r_flat():
        return flat[0], flat[1]

    def d_flat():
        return flat[2], flat[3]

    speed_ref = sound[0]
    for tissue in range(1, LABELS):
        speed_ref = jnp.maximum(speed_ref, sound[tissue])

    classes = lab[...].reshape(ROWS, NY)
    speed = jnp.full((ROWS, NY), sound[0])
    for tissue in range(1, LABELS):
        speed = jnp.where(classes == tissue, sound[tissue], speed)
    pressure = speed * speed * dens[...].reshape(ROWS, NY)
    put(P_S, product(r_flat, split(pressure), "nt"))
    pl.semaphore_wait(barrier, CHIPS)
    send(P_S)

    for load in loads[4:8]:
        load.wait()
    density_mass = jnp.full((ROWS, NY), mass[0])
    for tissue in range(1, LABELS):
        density_mass = jnp.where(classes == tissue, mass[tissue], density_mass)
    row = lax.broadcasted_iota(jnp.int32, (ROWS, NY), 0)
    col = lax.broadcasted_iota(jnp.int32, (ROWS, NY), 1)

    def damping(position, length):
        coordinate = position.astype(F32)
        depth = jnp.maximum(
            jnp.maximum(PML_W - coordinate, coordinate - (length - 1 - PML_W)), 0.0
        ) / PML_W
        square = depth * depth
        return jnp.exp(-ABSORB * speed_ref * (square * square) * DT * 0.5)

    damp = (
        damping(gz * Z_LOC + row // X_LOC, NZ),
        damping(gx * X_LOC + row % X_LOC, NX),
        damping(col, NY),
    )
    over_mass = DT / density_mass
    for a in range(3):
        base_v[a] = damp[a] * (damp[a] * vel[a].reshape(ROWS, NY))
        coef_v[a] = damp[a] * over_mass
    damp_all = damp[0] * damp[1] * damp[2]
    base_d[...] = damp_all * (damp_all * dens[...].reshape(ROWS, NY))
    coef_d[...] = damp_all * (DT * density_mass)

    line = lax.broadcasted_iota(jnp.int32, (256, NX), 0)
    index_x = lax.broadcasted_iota(jnp.int32, (256, NX), 1)

    def wave(index, length):
        folded = jnp.where(index <= length // 2, index, index - length // 2)
        return folded.astype(F32) * (2.0 * math.pi / length)

    folded = jnp.where(line <= 128 - core, line, line - 128)
    wz = (2 * folded + core).astype(F32) * (2.0 * math.pi / NZ)
    wx = wave(index_x, NX)
    wy = wave(jnp.full((256, NX), me, jnp.int32), NY)
    angle = speed_ref * jnp.sqrt(wz * wz + wx * wx + wy * wy) * (DT / 2.0)
    at_zero = angle == 0.0
    safe = jnp.where(at_zero, 1.0, angle)
    corr[...] = jnp.where(at_zero, 1.0, jnp.sin(safe) / safe)

    for load in loads[8:]:
        load.wait()
    for half in range(2):
        for table in range(4):
            turned_large[half, table] = large[half, table].T
    r_large, d_large = large.at[:, 0:2], large.at[:, 2:4]
    r_turned, d_turned = turned_large.at[:, 0:2], turned_large.at[:, 2:4]

    def r_mixed():
        return mixed[0], mixed[1]

    def d_mixed():
        return mixed[2], mixed[3]

    copies = []

    arrived(P_S)
    copy = give_half(P_C, lambda own: along_z(r_large, get_slab(P_S, own), own))
    copies.append(copy)
    spectrum = product(take_half(P_C, copy), r_mixed, "nt")
    spectrum = split(spectrum * corr[...])
    back_0, own_0 = give_back(V0_I, product(spectrum, r_mixed, "nn"))
    back_x, own_x = give_back(VX_I, product(spectrum, d_mixed, "nn"))
    copies += [back_0, back_x]
    part = along_z(r_turned, own_0, True)
    other_0 = take_back(V0_I, back_0)
    put_slab(U0_S, [part, along_z(r_turned, other_0, False)])
    send(U0_S)
    part = along_z(r_turned, own_x, True)
    put_slab(UX_S, [part, along_z(r_turned, take_back(VX_I, back_x), False)])
    send(UX_S)
    put_slab(UZ_S, [along_z(d_turned, own_0, True), along_z(d_turned, other_0, False)])
    send(UZ_S)

    where = sidx[...]
    plane = NX * NY
    z_off = where // plane - gz * Z_LOC
    remain = where % plane
    x_off = remain // NY - gx * X_LOC
    inside = (z_off >= 0) & (z_off < Z_LOC) & (x_off >= 0) & (x_off < X_LOC)
    row_of[...] = jnp.where(inside, z_off * X_LOC + x_off, -1)
    col_of[...] = remain % NY

    def add_some(step, carry):
        picks = []
        highs = []
        lows = []
        for part in range(2):
            at = pl.ds(step * 2 + part, 1)
            picks.append(jnp.where(row == row_of[at, :], 1.0, 0.0).astype(BF16))
            amount = jnp.where(row[:NY] == col_of[at, :], sval[at, :], 0.0)
            high, low = split(amount)
            highs.append(high)
            lows.append(low)
        pick = jnp.concatenate(picks, axis=1)
        contract = (((1,), (1,)), ((), ()))
        high = lax.dot_general(pick, jnp.concatenate(highs, axis=1), contract, preferred_element_type=F32)
        low = lax.dot_general(pick, jnp.concatenate(lows, axis=1), contract, preferred_element_type=F32)
        base_d[...] += high + low
        return carry

    lax.fori_loop(0, SRC // NY // 2, add_some, 0)

    for came, goes, a, back, sign in (
        (U0_S, VY_S, 2, d_flat, -1),
        (UX_S, VX_S, 1, r_flat, 1),
        (UZ_S, VZ_S, 0, r_flat, 1),
    ):
        arrived(came)
        slope = product(turned(came), back, "nn")
        fresh = base_v[a] - coef_v[a] * slope
        halves = split(fresh)
        if sign > 0:
            put(goes, product(r_flat, halves, "nt"))
        else:
            put(goes, -product(d_flat, halves, "nt"))
        send(goes)
        out_v[a] = fresh.reshape(Z_LOC, X_LOC, NY)

    arrived(VY_S)
    part_yz = [along_z(r_large, get_slab(VY_S, own), own) for own in (False, True)]
    arrived(VX_S)
    copy_x = give_half(X_C, lambda own: along_z(r_large, get_slab(VX_S, own), own))
    spectrum = product(take_half(X_C, copy_x), d_mixed, "nt")
    arrived(VZ_S)
    copy_yz = give_half(
        YZ_C, lambda own: part_yz[own] - along_z(d_large, get_slab(VZ_S, own), own)
    )
    spectrum = product(take_half(YZ_C, copy_yz), r_mixed, "nt") - spectrum
    back_e, own_e = give_back(E_I, product(split(spectrum * corr[...]), r_mixed, "nn"))
    copies += [copy_x, copy_yz, back_e]
    part = along_z(r_turned, own_e, True)
    put_slab(E_S, [part, along_z(r_turned, take_back(E_I, back_e), False)])
    send(E_S)

    arrived(E_S)
    spread = product(turned(E_S), r_flat, "nn")
    out_d[...] = (base_d[...] - coef_d[...] * spread).reshape(Z_LOC, X_LOC, NY)
    for which in range(8):
        sent(which)
    for copy in copies:
        copy.wait_send()


def write_out(new_d, new_v, out_d, out_v, out_sem):
    copies = [
        pltpu.make_async_copy(here, away, out_sem.at[i])
        for i, (here, away) in enumerate(
            [(new_v.at[a, pl.ds(h, 4)], out_v.at[a, pl.ds(h, 4)]) for a in range(3) for h in (0, 4)]
            + [(new_d.at[pl.ds(h, 4)], out_d.at[pl.ds(h, 4)]) for h in (0, 4)]
        )
    ]
    for copy in copies:
        copy.start()
    for copy in copies:
        copy.wait()


def shards(density, velocity, labels, sound_table, mass_table, source_index, source_values):
    small, large = tables()
    vmem = pl.BlockSpec(memory_space=pltpu.VMEM)
    hbm = pl.BlockSpec(memory_space=pl.ANY)
    field = (Z_LOC, X_LOC, NY)
    results = pl.pallas_call(
        kernel,
        out_shape=(
            pltpu.VMEM(field, F32),
            pltpu.VMEM((3,) + field, F32),
        ),
        in_specs=[hbm] * 9,
        out_specs=(vmem, vmem),
        scratch_shapes=[
            pltpu.VMEM((8, WIDE, 128), F32),
            pltpu.VMEM((8, WIDE, 128), F32),
            pltpu.VMEM((3, 128, 128), F32),
            pltpu.VMEM((3, 128, 128), F32),
            pltpu.VMEM((3, 128, 128), F32),
            pltpu.VMEM((3, 128, 128), F32),
            pltpu.VMEM((3, 128, 128), F32),
            pltpu.SMEM((LABELS,), F32),
            pltpu.SMEM((LABELS,), F32),
            pltpu.VMEM(field, F32),
            pltpu.VMEM((3,) + field, F32),
            pltpu.VMEM(field, jnp.int32),
            pltpu.VMEM((SRC // NY, NY), jnp.int32),
            pltpu.VMEM((SRC // NY, NY), F32),
            pltpu.VMEM((4, NX, NX), BF16),
            pltpu.VMEM((4, NX, NX), BF16),
            pltpu.VMEM((2, 4, NZ // 2, NZ // 2), BF16),
            pltpu.VMEM((2, 4, NZ // 2, NZ // 2), BF16),
            pltpu.VMEM((3, ROWS, NY), F32),
            pltpu.VMEM((3, ROWS, NY), F32),
            pltpu.VMEM((ROWS, NY), F32),
            pltpu.VMEM((ROWS, NY), F32),
            pltpu.VMEM((256, NX), F32),
            pltpu.VMEM((SRC // NY, NY), jnp.int32),
            pltpu.VMEM((SRC // NY, NY), jnp.int32),
            pltpu.SemaphoreType.DMA((8,)),
            pltpu.SemaphoreType.DMA((8,)),
            pltpu.SemaphoreType.DMA((3,)),
            pltpu.SemaphoreType.DMA((3,)),
            pltpu.SemaphoreType.DMA((3,)),
            pltpu.SemaphoreType.DMA((3,)),
            pltpu.SemaphoreType.DMA((10,)),
        ],
        compiler_params=pltpu.CompilerParams(collective_id=0, has_side_effects=True),
    )(
        sound_table,
        mass_table,
        density,
        velocity,
        labels,
        source_index.reshape(SRC // NY, NY),
        source_values[0].reshape(SRC // NY, NY),
        jnp.asarray(small),
        jnp.asarray(large),
    )

    return pl.pallas_call(
        write_out,
        out_shape=(
            jax.ShapeDtypeStruct(field, F32),
            jax.ShapeDtypeStruct((3,) + field, F32),
        ),
        in_specs=[vmem, vmem],
        out_specs=(hbm, hbm),
        scratch_shapes=[pltpu.SemaphoreType.DMA((8,))],
    )(*[pltpu.with_memory_space_constraint(result, pltpu.VMEM) for result in results])


def solution(mesh):
    in_specs = (
        P("gz", "gx", None),
        P(None, "gz", "gx", None),
        P("gz", "gx", None),
        P(),
        P(),
        P(),
        P(),
    )
    out_specs = (P("gz", "gx", None), P(None, "gz", "gx", None))
    return jax.shard_map(shards, mesh=mesh, in_specs=in_specs, out_specs=out_specs, check_vma=False)
```
